128 devices in a mesh: lon: 8 (over z, y_hi), lat: 16 (over y_lo, x, core).
Axes of the slice: x: 4, y: 4 (y_hi: 2, y_lo: 2; y = y_hi * 2 + y_lo), z: 4, core: 2. Of those that a mesh axis runs over, the one named last changes fastest.
Arguments:
- fields: float32 [4, 8, 1024, 3600], P(None, None, 'lat', 'lon'), may hold values from -6 to 6
- thickness: float32 [8], replicated, may hold values from 5 to 250
- cutoff: int32 [256], replicated, may hold values from 2 to 1800
- barotropic: float32 [3, 1024, 3600], P(None, 'lat', 'lon'), may hold values from -6 to 6
- land_sea: int32 [1024, 3600], P('lat', 'lon'), may hold values 0 or 1
Outputs:
- filtered_tracers: float32 [2, 8, 1024, 3600], P(None, None, 'lat', 'lon')
- velocity: float32 [2, 8, 1024, 3600], P(None, None, 'lat', 'lon')
- sea_level: float32 [1024, 3600], P('lat', 'lon')
The draws below stay inside these ranges and needn't reach their ends.
Inputs may be any that keep to these rules, and one draw needn't show every extreme that they name: `cutoff`: each filtered row's highest kept wavenumber.
All inputs are finite; a program needn't handle non-finite values. No bound on the sum of `land_sea` on one device may be relied on, other than what follows from the above.
Results may differ from the reference program's by a relative error of at most 0.0003.
Values sent between devices are 32-bit elements; how exact they have to be, the bound alone decides.
A program may use at most 128 MiB of HBM per device.

```python
import math
import jax
import jax.numpy as jnp
from jax import lax

NLON = 3600
LEV = 8
SUB = 20
NLAT = 1024
NPOLE = 128


def touch_ends(drawn, own_key, smallest, largest):
    extent = drawn.shape
    index_at = [jax.random.randint(jax.random.fold_in(own_key, axis), (), 0, extent[axis]) for axis in range(len(extent))]
    drawn = drawn.at[tuple(index_at)].set(smallest)
    longest = extent.index(max(extent))
    index_at[longest] = (index_at[longest] + 1) % extent[longest]
    return drawn.at[tuple(index_at)].set(largest)


def shard_levels(own_key, dims, split, least, top_value):
    def one(dim, shards_of):
        heights = jax.random.uniform(jax.random.fold_in(jax.random.fold_in(own_key, 6), dim), (shards_of,), jnp.float32, least / len(split), top_value / len(split))
        return jnp.repeat(jnp.exp(heights), dims[dim] // shards_of).reshape((-1,) + (1,) * (len(dims) - dim - 1))

    level = one(*split[0])
    for cut in split[1:]:
        level = level * one(*cut)
    return level


def gaussian(rng, dims, scale, most, shards=(), kind=jnp.bfloat16):
    drawn = scale * jax.random.normal(rng, dims, jnp.float32)
    if shards:
        drawn = drawn * shard_levels(rng, dims, shards, -0.22, 0.18)
    return jnp.clip(drawn, -most, most).astype(kind)


def setup_inputs(seed: int = 0) -> dict:
    arg_keys = jax.random.split(jax.random.key(seed), 6)
    fields = gaussian(arg_keys[0], (4, LEV, NLAT, NLON), 1.0, 6.0, ((2, 16), (3, 8)), jnp.float32)
    thickness = jnp.clip(jnp.exp(jax.random.uniform(arg_keys[1], (LEV,), jnp.float32, math.log(5.0), math.log(250.0))), 5.0, 250.0)
    cutoff = touch_ends(jax.random.randint(arg_keys[2], (2 * NPOLE,), 2, NLON // 2 + 1), jax.random.fold_in(arg_keys[2], 1), 2, (NLON // 2 + 1) - 1).astype(jnp.int32)
    barotropic = gaussian(arg_keys[3], (3, NLAT, NLON), 1.0, 6.0, ((1, 16), (2, 8)), jnp.float32)
    land_sea = touch_ends((jax.random.randint(arg_keys[4], (NLAT, NLON), 0, 5) < 4).astype(jnp.int32), jax.random.fold_in(arg_keys[4], 1), 0, 1)
    return {"fields": fields, "thickness": thickness, "cutoff": cutoff, "barotropic": barotropic, "land_sea": land_sea}


wave_coef = 0.65


def polar_filter(values, row_cuts):
    circle_len = values.shape[-1]
    spectrum = jnp.fft.rfft(values, axis=-1)
    wavenumber = jnp.arange(circle_len // 2 + 1)
    kept_mask = wavenumber[None, :] <= row_cuts[:, None]
    return jnp.fft.irfft(spectrum * kept_mask, n=circle_len, axis=-1).astype(values.dtype)


def reference(fields, thickness, cutoff, barotropic, land_sea):
    total_rows = fields.shape[2]
    pole_rows = cutoff.shape[0] // 2
    north_rows = polar_filter(fields[:, :, :pole_rows], cutoff[:pole_rows])
    south_rows = polar_filter(fields[:, :, total_rows - pole_rows:], cutoff[pole_rows:])
    filtered = jnp.concatenate([north_rows, fields[:, :, pole_rows:total_rows - pole_rows], south_rows], axis=2)
    ocean_cell = land_sea.astype(fields.dtype)
    row_number = jnp.arange(total_rows)
    east_open = ocean_cell * jnp.roll(ocean_cell, -1, 1)
    north_open = ocean_cell * jnp.roll(ocean_cell, -1, 0) * (row_number != total_rows - 1).astype(fields.dtype)[:, None]
    surface = barotropic[0]
    eastward = barotropic[1] * east_open
    northward = barotropic[2] * north_open
    for subcycle in range(SUB):
        divergence = eastward - jnp.roll(eastward, 1, 1) + northward - jnp.roll(northward, 1, 0)
        surface = surface - wave_coef * ocean_cell * divergence
        eastward = east_open * (eastward - wave_coef * (jnp.roll(surface, -1, 1) - surface))
        northward = north_open * (northward - wave_coef * (jnp.roll(surface, -1, 0) - surface))
    weights = thickness / jnp.sum(thickness)
    currents = filtered[2:]
    column = jnp.einsum("k,ckij->cij", weights, currents, precision=lax.Precision.HIGHEST)
    velocity = jnp.stack([east_open, north_open])[:, None] * (currents - column[:, None] + jnp.stack([eastward, northward])[:, None])
    return filtered[:2], velocity, surface
```

```python
import functools
import math

import jax
import jax.numpy as jnp
import ml_dtypes
import numpy as np
from jax import lax
from jax.experimental import pallas as pl
from jax.experimental.pallas import tpu as pltpu
from jax.sharding import PartitionSpec as P

MESH = pl.DeviceIdType.MESH
SUB = 20
COEF = 0.65
NLAT = 1024
NLON = 3600
ROWS = 64
COLS = 450
HALF = 32
HALO = 24
TILES = ((0, 128), (128, 256), (256, 384), (384, 450))
ROOT = math.sqrt(0.5)


def fourier_tables():
    k = np.arange(COLS)
    angle = 2.0 * np.pi * (np.outer(k, k) % COLS) / COLS
    both = np.zeros((512, 1024), np.float64)
    both[:COLS, :COLS] = np.cos(angle)
    both[:COLS, 512 : 512 + COLS] = np.sin(angle)
    high = both.astype(ml_dtypes.bfloat16)
    low = (both - high.astype(np.float64)).astype(ml_dtypes.bfloat16)
    twist = np.zeros((8, 512), np.float32)
    for j in range(1, 5):
        twist[2 * (j - 1), :COLS] = np.cos(2.0 * np.pi * j * k / NLON)
        twist[2 * (j - 1) + 1, :COLS] = np.sin(2.0 * np.pi * j * k / NLON)
    return np.stack([high, low]), twist


def place():
    lat = lax.axis_index("lat")
    lon = lax.axis_index("lon")
    ylo = lat // 8
    x = (lat % 8) // 2
    core = lat % 2
    xm = x + ylo * (3 - 2 * x)

    def peer(xm_to, lon_to):
        return {"lat": (ylo * 4 + xm_to + ylo * (3 - 2 * xm_to)) * 2 + core, "lon": lon_to}

    return lat, lon, ylo, core, xm, peer


def split_store(high, low, rows, cols, value):
    top = value.astype(jnp.bfloat16)
    high[rows, cols] = top
    low[rows, cols] = (value - top.astype(jnp.float32)).astype(jnp.bfloat16)


def transform(c, h, base, recv, ybuf, cut_ref, cutb, tw_ref, wv, high, low, acc):
    row_id = lax.broadcasted_iota(jnp.int32, (HALF, 128), 0)
    cuts = jnp.zeros((HALF, 128), jnp.int32)
    for r in range(HALF):
        cuts = jnp.where(row_id == r, cut_ref[base + h * HALF + r], cuts)
    cutb[...] = cuts

    def group(g, rb):
        return pl.ds(g * HALF + rb, 16)

    def product(rows):
        left, small = high[0:rows, :], low[0:rows, :]
        acc[0:rows, :] = (
            jnp.dot(left, wv[0], preferred_element_type=jnp.float32)
            + jnp.dot(small, wv[0], preferred_element_type=jnp.float32)
            + jnp.dot(left, wv[1], preferred_element_type=jnp.float32)
        )

    for rb in (0, 16):
        for lo, hi in TILES:
            cols = pl.ds(lo, hi - lo)
            x = [recv[c, d, pl.ds(rb, 16), cols] for d in range(8)]
            a = [x[d] + x[d + 4] for d in range(4)]
            b = [x[d] - x[d + 4] for d in range(4)]
            diff, total = ROOT * (b[1] - b[3]), ROOT * (b[1] + b[3])
            even, odd = a[0] + a[2], a[1] + a[3]
            real = {1: b[0] + diff, 2: a[0] - a[2], 3: b[0] - diff}
            imag = {1: -total - b[2], 2: a[3] - a[1], 3: b[2] - total}
            split_store(high, low, group(0, rb), cols, even + odd)
            for j in range(1, 5):
                tc = tw_ref[2 * j - 2 : 2 * j - 1, lo:hi]
                ts = tw_ref[2 * j - 1 : 2 * j, lo:hi]
                if j < 4:
                    zr = real[j] * tc + imag[j] * ts
                    zi = imag[j] * tc - real[j] * ts
                else:
                    zr = (even - odd) * tc
                    zi = (odd - even) * ts
                split_store(high, low, group(2 * j - 1, rb), cols, zr)
                split_store(high, low, group(2 * j, rb), cols, zi)
    product(9 * HALF)
    for rb in (0, 16):
        for lo, hi in TILES:
            cols = pl.ds(lo, hi - lo)
            sines = pl.ds(512 + lo, hi - lo)
            limit = cutb[pl.ds(rb, 16), 0 : hi - lo]
            step = 8 * (lax.broadcasted_iota(jnp.int32, (16, hi - lo), 1) + lo)
            for j in range(5):
                wave = step + j
                kept = jnp.minimum(wave, NLON - wave) <= limit
                scale = jnp.where(kept, (2.0 if 0 < j < 4 else 1.0) / NLON, 0.0)
                if j == 0:
                    re = acc[group(0, rb), cols]
                    im = -acc[group(0, rb), sines]
                else:
                    re = acc[group(2 * j - 1, rb), cols] + acc[group(2 * j, rb), sines]
                    im = acc[group(2 * j, rb), cols] - acc[group(2 * j - 1, rb), sines]
                split_store(high, low, group(2 * j, rb), cols, re * scale)
                split_store(high, low, group(2 * j + 1, rb), cols, im * scale)
    product(10 * HALF)
    for rb in (0, 16):
        for lo, hi in TILES:
            cols = pl.ds(lo, hi - lo)
            sines = pl.ds(512 + lo, hi - lo)
            hr, hm = {}, {}
            for j in range(5):
                gr = acc[group(2 * j, rb), cols] - acc[group(2 * j + 1, rb), sines]
                if j == 0:
                    hr[0] = gr
                    continue
                gi = acc[group(2 * j, rb), sines] + acc[group(2 * j + 1, rb), cols]
                tc = tw_ref[2 * j - 2 : 2 * j - 1, lo:hi]
                ts = tw_ref[2 * j - 1 : 2 * j, lo:hi]
                hr[j] = gr * tc - gi * ts
                if j < 4:
                    hm[j] = gr * ts + gi * tc
            even, odd = hr[0] + hr[4], hr[0] - hr[4]
            part = [even + hr[2], odd - hm[2], even - hr[2], odd + hm[2]]
            turn = [
                hr[1] + hr[3],
                ROOT * (hr[1] - hm[1] - hr[3] - hm[3]),
                hm[3] - hm[1],
                ROOT * (hr[3] - hm[3] - hr[1] - hm[1]),
            ]
            for d in range(4):
                ybuf[c, d, pl.ds(rb, 16), cols] = part[d] + turn[d]
                ybuf[c, d + 4, pl.ds(rb, 16), cols] = part[d] - turn[d]


def assemble(store, offset, count, centre, left, right, tail):
    rows = pl.ds(offset, count)
    store[rows, 0:COLS] = centre
    tail[0:count, 0:66] = left
    lane = lax.broadcasted_iota(jnp.int32, (count, 128), 1)
    own = store[rows, 384:512]
    west = pltpu.roll(tail[0:count, :], 62, 1)
    east = pltpu.roll(right, 66, 1)
    store[rows, 384:512] = jnp.where(
        lane < 66, own, jnp.where(lane < 66 + HALO, east, jnp.where(lane >= 128 - HALO, west, 0.0))
    )


def exchange_kernel(
    f_ref, baro_in, land_in, cut_in, w_ref, tw_in,
    filt, flow, opens,
    baro, land, cut_ref, tw_ref, recv, ybuf, crecv, wv, high, low, acc, cutb,
    state, masks, tail,
    lb, lm, rb_, rm, tb, tm, bb, bm, tlb, tlm, trb, trm, blb, blm, brb, brm,
    wsem, hsend, hrecv, rsem, osem, csend, crsem, dsend, fsem,
):
    lat, lon, ylo, core, xm, peer = place()
    lats, lons = 16, 8
    polar = xm == 0
    helper = (xm == 1) | (xm == 3)
    lat_up, lat_down = (lat + 1) % lats, (lat + lats - 1) % lats
    lon_up, lon_down = (lon + 1) % lons, (lon + lons - 1) % lons
    barrier = pltpu.get_barrier_semaphore()

    def greet(device):
        pl.semaphore_signal(barrier, 1, device_id=device, device_id_type=MESH)

    for device in ({"lat": lat_up, "lon": lon}, {"lat": lat_down, "lon": lon}, {"lat": lat, "lon": lon_up}, {"lat": lat, "lon": lon_down}):
        greet(device)

    @pl.when(polar)
    def _():
        for k in range(lons):
            to = (lon + k) % lons
            if k:
                greet(peer(0, to))
            greet(peer(1, to))
            greet(peer(3, to))

    @pl.when(helper)
    def _():
        for k in range(lons):
            to = (lon + k) % lons
            if k:
                greet(peer(xm, to))
            greet(peer(0, to))

    near = [
        pltpu.make_async_copy(baro_in, baro, wsem.at[0]),
        pltpu.make_async_copy(land_in, land, wsem.at[1]),
    ]
    tables = [
        pltpu.make_async_copy(cut_in, cut_ref, wsem.at[2]),
        pltpu.make_async_copy(tw_in, tw_ref, wsem.at[3]),
        pltpu.make_async_copy(w_ref, wv, wsem.at[4]),
    ]
    for copy in near + tables:
        copy.start()
    high[...] = jnp.zeros_like(high)
    low[...] = jnp.zeros_like(low)

    @pl.when(polar)
    def _():
        pl.semaphore_wait(barrier, 27)

    @pl.when(helper)
    def _():
        pl.semaphore_wait(barrier, 19)

    @pl.when(xm == 2)
    def _():
        pl.semaphore_wait(barrier, 4)

    def hop(i, source, target, **to):
        device = {"lat": lat, "lon": lon}
        device.update(to)
        return pltpu.make_async_remote_copy(source, target, hsend.at[i], hrecv.at[i], device_id=device, device_id_type=MESH)

    first = [
        hop(0, baro.at[:, :, pl.ds(384, 66)], lb, lon=lon_up),
        hop(1, land.at[:, pl.ds(384, 66)], lm, lon=lon_up),
        hop(2, baro.at[:, :, pl.ds(0, 128)], rb_, lon=lon_down),
        hop(3, land.at[:, pl.ds(0, 128)], rm, lon=lon_down),
        hop(4, baro.at[:, pl.ds(ROWS - HALO, HALO), :], tb, lat=lat_up),
        hop(5, land.at[pl.ds(ROWS - HALO, HALO), :], tm, lat=lat_up),
        hop(6, baro.at[:, pl.ds(0, HALO), :], bb, lat=lat_down),
        hop(7, land.at[pl.ds(0, HALO), :], bm, lat=lat_down),
    ]
    second = []
    for i, (source, flat, up, upm, down, downm) in enumerate(((lb, lm, tlb, tlm, blb, blm), (rb_, rm, trb, trm, brb, brm))):
        second += [
            hop(8 + 4 * i, source.at[:, pl.ds(ROWS - HALO, HALO), :], up, lat=lat_up),
            hop(9 + 4 * i, flat.at[pl.ds(ROWS - HALO, HALO), :], upm, lat=lat_up),
            hop(10 + 4 * i, source.at[:, pl.ds(0, HALO), :], down, lat=lat_down),
            hop(11 + 4 * i, flat.at[pl.ds(0, HALO), :], downm, lat=lat_down),
        ]
    for copy in near:
        copy.wait()
    for copy in first:
        copy.start()

    @pl.when(polar)
    def _():
        for h in range(2):
            rows = pl.ds(h * HALF, HALF)
            for s in range(2):
                pltpu.make_async_copy(f_ref.at[2 * lon + s, rows, :], recv.at[2 * h + s, lon], rsem.at[2 * h + s]).start()
            for k in range(lons):
                to = (lon + k) % lons

                def send(plane, c, xm_to):
                    pltpu.make_async_remote_copy(
                        f_ref.at[plane, rows, :], recv.at[c, lon], osem, rsem.at[c], device_id=peer(xm_to, to), device_id_type=MESH
                    ).start()

                send(16 + to, 2 * h, 1)
                send(24 + to, 2 * h, 3)
                if k:
                    send(2 * to, 2 * h, 0)
                    send(2 * to + 1, 2 * h + 1, 0)

    for copy in first[:4]:
        copy.wait_recv()
    for copy in second:
        copy.start()
    for copy in first[4:] + second:
        copy.wait_recv()

    for i in range(3):
        assemble(state.at[i], 0, HALO, tb[i], tlb[i], trb[i], tail)
        assemble(state.at[i], HALO, ROWS, baro[i], lb[i], rb_[i], tail)
        assemble(state.at[i], HALO + ROWS, HALO, bb[i], blb[i], brb[i], tail)
    f32 = jnp.float32
    assemble(masks.at[0], 0, HALO, tm[...].astype(f32), tlm[...].astype(f32), trm[...].astype(f32), tail)
    assemble(masks.at[0], HALO, ROWS, land[...].astype(f32), lm[...].astype(f32), rm[...].astype(f32), tail)
    assemble(masks.at[0], HALO + ROWS, HALO, bm[...].astype(f32), blm[...].astype(f32), brm[...].astype(f32), tail)
    total = ROWS + 2 * HALO
    for r in range(0, total, 8):
        rows = pl.ds(r, 8)
        sea = masks[0, rows, :]
        below = masks[0, pl.ds(r + 1, 8), :] if r + 8 < total else sea
        east = sea * pltpu.roll(sea, 511, 1)
        row = (lax.broadcasted_iota(jnp.int32, (8, 512), 0) + (r + NLAT - HALO) + lat * ROWS) % NLAT
        north = jnp.where(row == NLAT - 1, 0.0, sea * below)
        masks[1, rows, :] = east
        masks[2, rows, :] = north
        state[1, rows, :] = state[1, rows, :] * east
        state[2, rows, :] = state[2, rows, :] * north

    def cycle(_, carry):
        for r in range(0, total, 8):
            rows = pl.ds(r, 8)
            e, n = state[1, rows, :], state[2, rows, :]
            above = state[2, pl.ds(r - 1, 8), :] if r else n
            div = e - pltpu.roll(e, 1, 1) + n - above
            state[0, rows, :] = state[0, rows, :] - (COEF * masks[0, rows, :]) * div
        for r in range(0, total, 8):
            rows = pl.ds(r, 8)
            s = state[0, rows, :]
            below = state[0, pl.ds(r + 1, 8), :] if r + 8 < total else s
            state[1, rows, :] = masks[1, rows, :] * (state[1, rows, :] - COEF * (pltpu.roll(s, 511, 1) - s))
            state[2, rows, :] = masks[2, rows, :] * (state[2, rows, :] - COEF * (below - s))
        return carry

    lax.fori_loop(0, SUB, cycle, 0)
    flow[...] = state[:, pl.ds(HALO, ROWS), 0:COLS]
    opens[...] = masks[1:3, pl.ds(HALO, ROWS), 0:COLS]
    for copy in tables:
        copy.wait()

    base = ylo * 128 + core * ROWS
    stride = jnp.where(polar, 1, 2)

    def forward(h):
        pltpu.make_async_copy(crecv.at[0, pl.ds(0, 7)], crecv.at[0, pl.ds(0, 7)], crsem.at[h]).wait()
        rows = pl.ds(pl.multiple_of(h * HALF, HALF), HALF)
        for k in range(lons):
            origin = (lon + k) % lons
            source = crecv.at[h, origin] if k else ybuf.at[2 * h, lon]
            pltpu.make_async_remote_copy(
                source, filt.at[16 + 8 * (xm // 2) + origin, rows, :], dsend, fsem, device_id=peer(0, lon), device_id_type=MESH
            ).start()

    def chunk(i, carry):
        c = i * stride
        h = c // 2
        rows = pl.ds(pl.multiple_of(h * HALF, HALF), HALF)
        pltpu.make_async_copy(recv.at[c], recv.at[c], rsem.at[c]).wait()
        transform(c, h, base, recv, ybuf, cut_ref, cutb, tw_ref, wv, high, low, acc)

        @pl.when(polar)
        def _():
            plane = 2 * lon + c % 2
            pltpu.make_async_copy(ybuf.at[c, lon], filt.at[plane, rows, :], fsem).start()
            for k in range(1, lons):
                to = (lon + k) % lons
                pltpu.make_async_remote_copy(
                    ybuf.at[c, to], filt.at[plane, rows, :], csend, fsem, device_id=peer(0, to), device_id_type=MESH
                ).start()

        @pl.when(helper)
        def _():
            for k in range(1, lons):
                to = (lon + k) % lons
                pltpu.make_async_remote_copy(
                    ybuf.at[c, to], crecv.at[h, lon], csend, crsem.at[h], device_id=peer(xm, to), device_id_type=MESH
                ).start()

            @pl.when(i > 0)
            def _():
                forward(h - 1)

        return carry

    lax.fori_loop(0, jnp.where(polar, 4, jnp.where(helper, 2, 0)), chunk, 0)

    def drain(planes, sem):
        pltpu.make_async_copy(f_ref.at[pl.ds(0, planes)], f_ref.at[pl.ds(0, planes)], sem).wait()

    @pl.when(helper)
    def _():
        forward(1)
        drain(7, csend)
        drain(8, dsend)

    @pl.when(polar)
    def _():
        drain(30, osem)
        drain(14, csend)
        drain(32, fsem)

    for copy in first + second:
        copy.wait_send()


def finish_kernel(thick, f_ref, filt, flow, opens, tracers, velocity, sea, block, made, isem, tsem, vsem):
    lat, lon, ylo, core, xm, peer = place()
    polar = xm == 0
    order = (2, 3, 0, 1)

    def load(source):
        for g in order:
            pltpu.make_async_copy(source.at[pl.ds(8 * g, 8)], block.at[pl.ds(8 * g, 8)], isem.at[g]).start()

    @pl.when(polar)
    def _():
        load(filt)

    @pl.when(jnp.logical_not(polar))
    def _():
        load(f_ref)

    sea[...] = flow[0]
    weight = [thick[k] for k in range(8)]
    whole = functools.reduce(lambda a, b: a + b, weight)
    outs = []
    for c in range(2):
        part = pl.ds(16 + 8 * c, 8)
        pltpu.make_async_copy(f_ref.at[part], block.at[part], isem.at[2 + c]).wait()
        for r in range(0, ROWS, 8):
            rows = pl.ds(r, 8)
            level = [block[16 + 8 * c + k, rows, :] for k in range(8)]
            column = weight[0] * level[0]
            for k in range(1, 8):
                column = column + weight[k] * level[k]
            column = flow[1 + c, rows, :] - column / jnp.full((8, COLS), whole, jnp.float32)
            gate = opens[c, rows, :]
            for k in range(8):
                made[8 * c + k, rows, :] = gate * (level[k] + column)
        outs.append(pltpu.make_async_copy(made.at[pl.ds(8 * c, 8)], velocity.at[pl.ds(8 * c, 8)], vsem.at[c]))
        outs[-1].start()
    for g in range(2):
        part = pl.ds(8 * g, 8)
        pltpu.make_async_copy(f_ref.at[part], block.at[part], isem.at[g]).wait()
        outs.append(pltpu.make_async_copy(block.at[part], tracers.at[part], tsem.at[g]))
        outs[-1].start()
    for copy in outs:
        copy.wait()


def body(fields, thickness, cutoff, barotropic, land_sea):
    f32, i32, bf16 = jnp.float32, jnp.int32, jnp.bfloat16
    planes = fields.reshape(32, ROWS, COLS)
    table, twist = fourier_tables()
    hbm = pl.BlockSpec(memory_space=pltpu.HBM)
    vmem = pl.BlockSpec(memory_space=pltpu.VMEM)
    smem = pl.BlockSpec(memory_space=pltpu.SMEM)
    dma = pltpu.SemaphoreType.DMA
    strips = []
    for rows in (ROWS,):
        strips += [pltpu.VMEM((3, rows, 66), f32), pltpu.VMEM((rows, 66), i32), pltpu.VMEM((3, rows, 128), f32), pltpu.VMEM((rows, 128), i32)]
    strips += [pltpu.VMEM((3, HALO, COLS), f32), pltpu.VMEM((HALO, COLS), i32)] * 2
    strips += [pltpu.VMEM((3, HALO, 66), f32), pltpu.VMEM((HALO, 66), i32), pltpu.VMEM((3, HALO, 128), f32), pltpu.VMEM((HALO, 128), i32)] * 2
    total = ROWS + 2 * HALO
    filt, flow, opens = pl.pallas_call(
        exchange_kernel,
        out_shape=(
            jax.ShapeDtypeStruct((32, ROWS, COLS), f32),
            jax.ShapeDtypeStruct((3, ROWS, COLS), f32),
            jax.ShapeDtypeStruct((2, ROWS, COLS), f32),
        ),
        in_specs=[hbm] * 6,
        out_specs=(hbm, vmem, vmem),
        scratch_shapes=[
            pltpu.VMEM((3, ROWS, COLS), f32),
            pltpu.VMEM((ROWS, COLS), i32),
            pltpu.SMEM((256,), i32),
            pltpu.VMEM((8, 512), f32),
            pltpu.VMEM((4, 8, HALF, COLS), f32),
            pltpu.VMEM((4, 8, HALF, COLS), f32),
            pltpu.VMEM((2, 8, HALF, COLS), f32),
            pltpu.VMEM((2, 512, 1024), bf16),
            pltpu.VMEM((10 * HALF, 512), bf16),
            pltpu.VMEM((10 * HALF, 512), bf16),
            pltpu.VMEM((10 * HALF, 1024), f32),
            pltpu.VMEM((HALF, 128), i32),
            pltpu.VMEM((3, total, 512), f32),
            pltpu.VMEM((3, total, 512), f32),
            pltpu.VMEM((ROWS, 128), f32),
            *strips,
            dma((5,)), dma((16,)), dma((16,)), dma((4,)), dma, dma, dma((2,)), dma, dma,
        ],
        compiler_params=pltpu.CompilerParams(collective_id=1, has_side_effects=True, vmem_limit_bytes=67043328),
    )(planes, barotropic, land_sea, cutoff, jnp.asarray(table), jnp.asarray(twist))
    tracers, velocity, sea = pl.pallas_call(
        finish_kernel,
        out_shape=(
            jax.ShapeDtypeStruct((16, ROWS, COLS), f32),
            jax.ShapeDtypeStruct((16, ROWS, COLS), f32),
            jax.ShapeDtypeStruct((ROWS, COLS), f32),
        ),
        in_specs=[smem, hbm, hbm, vmem, vmem],
        out_specs=(hbm, hbm, vmem),
        scratch_shapes=[pltpu.VMEM((32, ROWS, COLS), f32), pltpu.VMEM((16, ROWS, COLS), f32), dma((4,)), dma((2,)), dma((2,))],
        compiler_params=pltpu.CompilerParams(vmem_limit_bytes=67043328),
    )(thickness, planes, filt, flow, opens)
    shape = (2, 8, ROWS, COLS)
    return tracers.reshape(shape), velocity.reshape(shape), sea


def solution(mesh):
    return jax.shard_map(
        body,
        mesh=mesh,
        in_specs=(P(None, None, "lat", "lon"), P(), P(), P(None, "lat", "lon"), P("lat", "lon")),
        out_specs=(P(None, None, "lat", "lon"), P(None, None, "lat", "lon"), P("lat", "lon")),
        check_vma=False,
    )
```

```python
import functools
import math

import jax
import jax.numpy as jnp
import ml_dtypes
import numpy as np
from jax import lax
from jax.experimental import pallas as pl
from jax.experimental.pallas import tpu as pltpu
from jax.sharding import PartitionSpec as P

MESH = pl.DeviceIdType.MESH
SUB = 20
COEF = 0.65
NLAT = 1024
NLON = 3600
ROWS = 64
COLS = 450
PART = 8
EACH = ROWS // PART
TAKES = (14, 9, 0, 9)
STARTS = (0, 112, 184, 184)
LAG = 2
AHEAD = 4
HALO = 24
TILES = ((0, 128), (128, 256), (256, 384), (384, 450))
ROOT = math.sqrt(0.5)


def fourier_tables():
    k = np.arange(COLS)
    angle = 2.0 * np.pi * (np.outer(k, k) % COLS) / COLS
    both = np.zeros((512, 1024), np.float64)
    both[:COLS, :COLS] = np.cos(angle)
    both[:COLS, 512 : 512 + COLS] = np.sin(angle)
    high = both.astype(ml_dtypes.bfloat16)
    low = (both - high.astype(np.float64)).astype(ml_dtypes.bfloat16)
    twist = np.zeros((8, 512), np.float32)
    for j in range(1, 5):
        twist[2 * (j - 1), :COLS] = np.cos(2.0 * np.pi * j * k / NLON)
        twist[2 * (j - 1) + 1, :COLS] = np.sin(2.0 * np.pi * j * k / NLON)
    return np.stack([high, low]), twist


def place():
    lat = lax.axis_index("lat")
    lon = lax.axis_index("lon")
    ylo = lat // 8
    x = (lat % 8) // 2
    core = lat % 2
    xm = x + ylo * (3 - 2 * x)

    def peer(xm_to, lon_to):
        return {"lat": (ylo * 4 + xm_to + ylo * (3 - 2 * xm_to)) * 2 + core, "lon": lon_to}

    return lat, lon, ylo, core, xm, peer


def split_store(terms, j, cols, real, imag):
    value = jnp.concatenate([real, imag], axis=0)
    top = value.astype(jnp.bfloat16)
    terms[pl.ds(2 * PART * j, 2 * PART), cols] = top
    terms[pl.ds(10 * PART + 2 * PART * j, 2 * PART), cols] = (value - top.astype(jnp.float32)).astype(jnp.bfloat16)


def transform(c, base, recv, ybuf, cut_ref, cutb, tw_ref, wv, terms, acc):
    row_id = lax.broadcasted_iota(jnp.int32, (PART, 128), 0)
    cuts = jnp.zeros((PART, 128), jnp.int32)
    for r in range(PART):
        cuts = jnp.where(row_id == r, cut_ref[base + r], cuts)
    cutb[...] = cuts

    def product():
        both = jnp.dot(terms[...], wv[0], preferred_element_type=jnp.float32)
        fine = jnp.dot(terms[0 : 10 * PART, :], wv[1], preferred_element_type=jnp.float32)
        acc[...] = both[0 : 10 * PART] + both[10 * PART :] + fine

    def part(j, imag, cols):
        return acc[pl.ds(2 * PART * j + PART * imag, PART), cols]

    for lo, hi in TILES:
        cols = pl.ds(lo, hi - lo)
        x = [recv[c, d, :, cols] for d in range(8)]
        a = [x[d] + x[d + 4] for d in range(4)]
        b = [x[d] - x[d + 4] for d in range(4)]
        diff, total = ROOT * (b[1] - b[3]), ROOT * (b[1] + b[3])
        even, odd = a[0] + a[2], a[1] + a[3]
        real = {1: b[0] + diff, 2: a[0] - a[2], 3: b[0] - diff}
        imag = {1: -total - b[2], 2: a[3] - a[1], 3: b[2] - total}
        split_store(terms, 0, cols, even + odd, jnp.zeros_like(even))
        for j in range(1, 5):
            tc = tw_ref[2 * j - 2 : 2 * j - 1, lo:hi]
            ts = tw_ref[2 * j - 1 : 2 * j, lo:hi]
            if j < 4:
                split_store(terms, j, cols, real[j] * tc + imag[j] * ts, imag[j] * tc - real[j] * ts)
            else:
                split_store(terms, j, cols, (even - odd) * tc, (odd - even) * ts)
    product()
    for lo, hi in TILES:
        cols = pl.ds(lo, hi - lo)
        sines = pl.ds(512 + lo, hi - lo)
        limit = cutb[:, 0 : hi - lo]
        step = 8 * (lax.broadcasted_iota(jnp.int32, (PART, hi - lo), 1) + lo)
        for j in range(5):
            wave = step + j
            kept = jnp.minimum(wave, NLON - wave) <= limit
            scale = jnp.where(kept, (2.0 if 0 < j < 4 else 1.0) / NLON, 0.0)
            re = part(j, 0, cols) + part(j, 1, sines)
            im = part(j, 1, cols) - part(j, 0, sines)
            split_store(terms, j, cols, re * scale, im * scale)
    product()
    for lo, hi in TILES:
        cols = pl.ds(lo, hi - lo)
        sines = pl.ds(512 + lo, hi - lo)
        hr, hm = {}, {}
        for j in range(5):
            gr = part(j, 0, cols) - part(j, 1, sines)
            if j == 0:
                hr[0] = gr
                continue
            gi = part(j, 0, sines) + part(j, 1, cols)
            tc = tw_ref[2 * j - 2 : 2 * j - 1, lo:hi]
            ts = tw_ref[2 * j - 1 : 2 * j, lo:hi]
            hr[j] = gr * tc - gi * ts
            if j < 4:
                hm[j] = gr * ts + gi * tc
        even, odd = hr[0] + hr[4], hr[0] - hr[4]
        plain = [even + hr[2], odd - hm[2], even - hr[2], odd + hm[2]]
        turn = [
            hr[1] + hr[3],
            ROOT * (hr[1] - hm[1] - hr[3] - hm[3]),
            hm[3] - hm[1],
            ROOT * (hr[3] - hm[3] - hr[1] - hm[1]),
        ]
        for d in range(4):
            ybuf[c, d, :, cols] = plain[d] + turn[d]
            ybuf[c, d + 4, :, cols] = plain[d] - turn[d]


def assemble(store, offset, count, centre, left, right, tail):
    rows = pl.ds(offset, count)
    store[rows, 0:COLS] = centre
    tail[0:count, 0:66] = left
    lane = lax.broadcasted_iota(jnp.int32, (count, 128), 1)
    own = store[rows, 384:512]
    west = pltpu.roll(tail[0:count, :], 62, 1)
    east = pltpu.roll(right, 66, 1)
    store[rows, 384:512] = jnp.where(
        lane < 66, own, jnp.where(lane < 66 + HALO, east, jnp.where(lane >= 128 - HALO, west, 0.0))
    )


def exchange_kernel(
    f_ref, baro_in, land_in, cut_in, w_ref, tw_in,
    filt, flow, opens,
    baro, land, cut_ref, tw_ref, recv, ybuf, crecv, wv, terms, acc, cutb,
    state, masks, tail, held_flow, held_opens,
    lb, lm, rb_, rm, tb, tm, bb, bm, tlb, tlm, trb, trm, blb, blm, brb, brm,
    wsem, hsend, hrecv, rsem, osem, csend, crsem, dsend, fsem,
):
    lat, lon, ylo, core, xm, peer = place()
    lats, lons = 16, 8
    polar = xm == 0
    helper = (xm == 1) | (xm == 3)
    lat_up, lat_down = (lat + 1) % lats, (lat + lats - 1) % lats
    lon_up, lon_down = (lon + 1) % lons, (lon + lons - 1) % lons
    barrier = pltpu.get_barrier_semaphore()

    def greet(device):
        pl.semaphore_signal(barrier, 1, device_id=device, device_id_type=MESH)

    for lat_to in (lat, lat_up, lat_down):
        for lon_to in (lon, lon_up, lon_down):
            if lat_to is not lat or lon_to is not lon:
                greet({"lat": lat_to, "lon": lon_to})

    @pl.when(polar)
    def _():
        for k in range(lons):
            to = (lon + k) % lons
            if k:
                greet(peer(0, to))
            greet(peer(1, to))
            greet(peer(3, to))

    @pl.when(helper)
    def _():
        for k in range(lons):
            to = (lon + k) % lons
            if k:
                greet(peer(xm, to))
            greet(peer(0, to))

    near = [
        pltpu.make_async_copy(baro_in, baro, wsem.at[0]),
        pltpu.make_async_copy(land_in, land, wsem.at[1]),
    ]
    tables = [
        pltpu.make_async_copy(cut_in, cut_ref, wsem.at[2]),
        pltpu.make_async_copy(tw_in, tw_ref, wsem.at[3]),
        pltpu.make_async_copy(w_ref, wv, wsem.at[4]),
    ]
    for copy in near + tables:
        copy.start()
    terms[...] = jnp.zeros_like(terms)

    @pl.when(polar)
    def _():
        pl.semaphore_wait(barrier, 31)

    @pl.when(helper)
    def _():
        pl.semaphore_wait(barrier, 23)

    @pl.when(xm == 2)
    def _():
        pl.semaphore_wait(barrier, 8)

    def hop(i, source, target, **to):
        device = {"lat": lat, "lon": lon}
        device.update(to)
        return pltpu.make_async_remote_copy(source, target, hsend.at[i], hrecv.at[i], device_id=device, device_id_type=MESH)

    first = [
        hop(0, baro.at[:, :, pl.ds(384, 66)], lb, lon=lon_up),
        hop(1, land.at[:, pl.ds(384, 66)], lm, lon=lon_up),
        hop(2, baro.at[:, :, pl.ds(0, 128)], rb_, lon=lon_down),
        hop(3, land.at[:, pl.ds(0, 128)], rm, lon=lon_down),
        hop(4, baro.at[:, pl.ds(ROWS - HALO, HALO), :], tb, lat=lat_up),
        hop(5, land.at[pl.ds(ROWS - HALO, HALO), :], tm, lat=lat_up),
        hop(6, baro.at[:, pl.ds(0, HALO), :], bb, lat=lat_down),
        hop(7, land.at[pl.ds(0, HALO), :], bm, lat=lat_down),
    ]
    low_rows, top_rows = pl.ds(ROWS - HALO, HALO), pl.ds(0, HALO)
    west_cols, east_cols = pl.ds(384, 66), pl.ds(0, 128)
    corners = ((low_rows, lat_up, tlb, tlm, trb, trm), (top_rows, lat_down, blb, blm, brb, brm))
    for i, (part, lat_to, left, leftm, right, rightm) in enumerate(corners):
        first += [
            hop(8 + 4 * i, baro.at[:, part, west_cols], left, lat=lat_to, lon=lon_up),
            hop(9 + 4 * i, land.at[part, west_cols], leftm, lat=lat_to, lon=lon_up),
            hop(10 + 4 * i, baro.at[:, part, east_cols], right, lat=lat_to, lon=lon_down),
            hop(11 + 4 * i, land.at[part, east_cols], rightm, lat=lat_to, lon=lon_down),
        ]
    for copy in near:
        copy.wait()
    for copy in first:
        copy.start()

    def chunk_of(xm_of, lon_of, i):
        unit = STARTS[xm_of] + lon_of * TAKES[xm_of] + i
        return unit // EACH, pl.ds(pl.multiple_of(unit % EACH * PART, PART), PART)

    def drain(chunks, sem):
        if chunks // EACH:
            whole = f_ref.at[pl.ds(0, chunks // EACH)]
            pltpu.make_async_copy(whole, whole, sem).wait()
        if chunks % EACH:
            rest = f_ref.at[0, pl.ds(0, chunks % EACH * PART), :]
            pltpu.make_async_copy(rest, rest, sem).wait()

    def settle(i):
        drain(7 + 16 * (i < TAKES[1]), osem.at[i])

    def deal(i):
        plane, rows = chunk_of(0, lon, i)
        pltpu.make_async_copy(f_ref.at[plane, rows, :], recv.at[i, lon], rsem.at[i]).start()

        def one(k, carry):
            to = (lon + k) % lons

            def send(xm_to):
                plane, rows = chunk_of(xm_to, to, i)
                pltpu.make_async_remote_copy(
                    f_ref.at[plane, rows, :], recv.at[i, lon], osem.at[i], rsem.at[i], device_id=peer(xm_to, to), device_id_type=MESH
                ).start()

            if i < TAKES[1]:
                send(1)
                send(3)

            @pl.when(k > 0)
            def _():
                send(0)

            return carry

        lax.fori_loop(0, lons, one, 0)

    @pl.when(polar)
    def _():
        for i in range(AHEAD):
            deal(i)

    for copy in first:
        copy.wait_recv()

    for i in range(3):
        assemble(state.at[i], 0, HALO, tb[i], tlb[i], trb[i], tail)
        assemble(state.at[i], HALO, ROWS, baro[i], lb[i], rb_[i], tail)
        assemble(state.at[i], HALO + ROWS, HALO, bb[i], blb[i], brb[i], tail)
    f32 = jnp.float32
    assemble(masks.at[0], 0, HALO, tm[...].astype(f32), tlm[...].astype(f32), trm[...].astype(f32), tail)
    assemble(masks.at[0], HALO, ROWS, land[...].astype(f32), lm[...].astype(f32), rm[...].astype(f32), tail)
    assemble(masks.at[0], HALO + ROWS, HALO, bm[...].astype(f32), blm[...].astype(f32), brm[...].astype(f32), tail)
    total = ROWS + 2 * HALO
    for r in range(0, total, 8):
        rows = pl.ds(r, 8)
        sea = masks[0, rows, :]
        below = masks[0, pl.ds(r + 1, 8), :] if r + 8 < total else sea
        east = sea * pltpu.roll(sea, 511, 1)
        row = (lax.broadcasted_iota(jnp.int32, (8, 512), 0) + (r + NLAT - HALO) + lat * ROWS) % NLAT
        north = jnp.where(row == NLAT - 1, 0.0, sea * below)
        masks[1, rows, :] = east
        masks[2, rows, :] = north
        state[1, rows, :] = state[1, rows, :] * east
        state[2, rows, :] = state[2, rows, :] * north

    def cycle(_, carry):
        for r in range(0, total, 8):
            rows = pl.ds(r, 8)
            e, n = state[1, rows, :], state[2, rows, :]
            above = state[2, pl.ds(r - 1, 8), :] if r else n
            div = e - pltpu.roll(e, 1, 1) + n - above
            state[0, rows, :] = state[0, rows, :] - (COEF * masks[0, rows, :]) * div
        for r in range(0, total, 8):
            rows = pl.ds(r, 8)
            s = state[0, rows, :]
            below = state[0, pl.ds(r + 1, 8), :] if r + 8 < total else s
            state[1, rows, :] = masks[1, rows, :] * (state[1, rows, :] - COEF * (pltpu.roll(s, 511, 1) - s))
            state[2, rows, :] = masks[2, rows, :] * (state[2, rows, :] - COEF * (below - s))
        return carry

    for copy in tables:
        copy.wait()

    base = ylo * 128 + core * ROWS
    far = xm // 2
    start = STARTS[1] + (STARTS[3] - STARTS[1]) * far

    def forward(i):
        pltpu.make_async_copy(crecv.at[0, pl.ds(0, 7)], crecv.at[0, pl.ds(0, 7)], crsem.at[i]).wait()

        def to_polar(source, origin):
            unit = start + origin * TAKES[1] + i
            rows = pl.ds(pl.multiple_of(unit % EACH * PART, PART), PART)
            pltpu.make_async_remote_copy(
                source, filt.at[unit // EACH, rows, :], dsend, fsem, device_id=peer(0, lon), device_id_type=MESH
            ).start()

        to_polar(ybuf.at[i, lon], lon)

        def relay(k, carry):
            origin = (lon + k) % lons
            to_polar(crecv.at[i, origin], origin)
            return carry

        lax.fori_loop(1, lons, relay, 0)

    @pl.when(polar)
    def _():
        for i in range(2):
            settle(i)
            deal(i + AHEAD)

    def chunk(i, carry):
        unit = jnp.where(polar, lon * TAKES[0], start + lon * TAKES[1]) + i
        plane = unit // EACH
        row = pl.multiple_of(unit % EACH * PART, PART)

        @pl.when(polar | helper)
        def _():
            pltpu.make_async_copy(recv.at[i], recv.at[i], rsem.at[i]).wait()
            transform(i, base + row, recv, ybuf, cut_ref, cutb, tw_ref, wv, terms, acc)

        @pl.when(polar)
        def _():
            target = filt.at[plane, pl.ds(row, PART), :]
            pltpu.make_async_copy(ybuf.at[i, lon], target, fsem).start()

            def back(k, carry):
                to = (lon + k) % lons
                pltpu.make_async_remote_copy(ybuf.at[i, to], target, csend, fsem, device_id=peer(0, to), device_id_type=MESH).start()
                return carry

            lax.fori_loop(1, lons, back, 0)
            for g in range(TAKES[0] - AHEAD - 2):

                @pl.when(i == g)
                def _():
                    settle(g + 2)
                    deal(g + 2 + AHEAD)

        @pl.when(helper)
        def _():
            def swap(k, carry):
                to = (lon + k) % lons
                pltpu.make_async_remote_copy(
                    ybuf.at[i, to], crecv.at[i, lon], csend, crsem.at[i], device_id=peer(xm, to), device_id_type=MESH
                ).start()
                return carry

            lax.fori_loop(1, lons, swap, 0)

        lax.fori_loop(0, jnp.where(i < TAKES[1], SUB // TAKES[1], 0) + jnp.where(i < SUB % TAKES[1], 1, 0), cycle, 0)

        @pl.when(helper & (i >= LAG))
        def _():
            forward(i - LAG)

        return carry

    lax.fori_loop(0, jnp.where(polar, TAKES[0], TAKES[1]), chunk, 0)
    held_flow[...] = state[:, pl.ds(HALO, ROWS), 0:COLS]
    held_opens[...] = masks[1:3, pl.ds(HALO, ROWS), 0:COLS]
    made = [pltpu.make_async_copy(held_flow, flow, wsem.at[0]), pltpu.make_async_copy(held_opens, opens, wsem.at[1])]
    for copy in made:
        copy.start()

    @pl.when(helper)
    def _():
        for i in range(TAKES[1] - LAG, TAKES[1]):
            forward(i)
        drain(7 * TAKES[1], csend)
        drain(8 * TAKES[1], dsend)

    @pl.when(polar)
    def _():
        for i in range(TAKES[0] - AHEAD, TAKES[0]):
            settle(i)
        drain(7 * TAKES[0], csend)
        drain(32 * EACH, fsem)

    for copy in made:
        copy.wait()
    for copy in first:
        copy.wait_send()


def finish_kernel(thick_in, f_ref, filt, flow_in, opens_in, tracers, velocity, sea, thick, flow, opens, block, made, isem, tsem, vsem, wsem):
    lat, lon, ylo, core, xm, peer = place()
    polar = xm == 0
    pieces = [(q, g) for q in range(4) for g in (2, 3, 0, 1)]

    def view(ref, q, g):
        return ref.at[pl.ds(8 * g, 8), pl.ds(16 * q, 16), :]

    def load(source):
        for q, g in pieces:
            pltpu.make_async_copy(view(source, q, g), view(block, q, g), isem.at[q, g]).start()

    @pl.when(polar)
    def _():
        load(filt)

    @pl.when(jnp.logical_not(polar))
    def _():
        load(f_ref)

    small = [pltpu.make_async_copy(flow_in, flow, wsem.at[0]), pltpu.make_async_copy(opens_in, opens, wsem.at[1]), pltpu.make_async_copy(thick_in, thick, wsem.at[3])]
    for copy in small:
        copy.start()
    for copy in small:
        copy.wait()
    weight = [thick[k] for k in range(8)]
    whole = functools.reduce(lambda a, b: a + b, weight)
    share = 1.0 / jnp.full((8, COLS), whole, jnp.float32)
    outs = [pltpu.make_async_copy(flow.at[0], sea, wsem.at[2])]
    outs[0].start()
    for q, g in pieces:
        pltpu.make_async_copy(view(f_ref, q, g), view(block, q, g), isem.at[q, g]).wait()
        if g < 2:
            outs.append(pltpu.make_async_copy(view(block, q, g), view(tracers, q, g), tsem.at[q, g]))
        else:
            c = g - 2
            for r in range(16 * q, 16 * q + 16, 8):
                rows = pl.ds(r, 8)
                level = [block[8 * g + k, rows, :] for k in range(8)]
                column = weight[0] * level[0]
                for k in range(1, 8):
                    column = column + weight[k] * level[k]
                column = flow[1 + c, rows, :] - column * share
                gate = opens[c, rows, :]
                for k in range(8):
                    made[8 * c + k, rows, :] = gate * (level[k] + column)
            outs.append(pltpu.make_async_copy(view(made, q, c), view(velocity, q, c), vsem.at[q, c]))
        outs[-1].start()
    for copy in outs:
        copy.wait()


def body(fields, thickness, cutoff, barotropic, land_sea):
    f32, i32, bf16 = jnp.float32, jnp.int32, jnp.bfloat16
    planes = fields.reshape(32, ROWS, COLS)
    table, twist = fourier_tables()
    hbm = pl.BlockSpec(memory_space=pltpu.HBM)
    dma = pltpu.SemaphoreType.DMA
    strips = []
    for rows in (ROWS,):
        strips += [pltpu.VMEM((3, rows, 66), f32), pltpu.VMEM((rows, 66), i32), pltpu.VMEM((3, rows, 128), f32), pltpu.VMEM((rows, 128), i32)]
    strips += [pltpu.VMEM((3, HALO, COLS), f32), pltpu.VMEM((HALO, COLS), i32)] * 2
    strips += [pltpu.VMEM((3, HALO, 66), f32), pltpu.VMEM((HALO, 66), i32), pltpu.VMEM((3, HALO, 128), f32), pltpu.VMEM((HALO, 128), i32)] * 2
    total = ROWS + 2 * HALO
    filt, flow, opens = pl.pallas_call(
        exchange_kernel,
        out_shape=(
            jax.ShapeDtypeStruct((32, ROWS, COLS), f32),
            jax.ShapeDtypeStruct((3, ROWS, COLS), f32),
            jax.ShapeDtypeStruct((2, ROWS, COLS), f32),
        ),
        in_specs=[hbm] * 6,
        out_specs=(hbm, hbm, hbm),
        scratch_shapes=[
            pltpu.VMEM((3, ROWS, COLS), f32),
            pltpu.VMEM((ROWS, COLS), i32),
            pltpu.SMEM((256,), i32),
            pltpu.VMEM((8, 512), f32),
            pltpu.VMEM((TAKES[0], 8, PART, COLS), f32),
            pltpu.VMEM((TAKES[0], 8, PART, COLS), f32),
            pltpu.VMEM((TAKES[1], 8, PART, COLS), f32),
            pltpu.VMEM((2, 512, 1024), bf16),
            pltpu.VMEM((20 * PART, 512), bf16),
            pltpu.VMEM((10 * PART, 1024), f32),
            pltpu.VMEM((PART, 128), i32),
            pltpu.VMEM((3, total, 512), f32),
            pltpu.VMEM((3, total, 512), f32),
            pltpu.VMEM((ROWS, 128), f32),
            pltpu.VMEM((3, ROWS, COLS), f32),
            pltpu.VMEM((2, ROWS, COLS), f32),
            *strips,
            dma((5,)), dma((16,)), dma((16,)), dma((TAKES[0],)), dma((TAKES[0],)), dma, dma((TAKES[1],)), dma, dma,
        ],
        compiler_params=pltpu.CompilerParams(collective_id=1, has_side_effects=True, vmem_limit_bytes=67043328),
    )(planes, barotropic, land_sea, cutoff, jnp.asarray(table), jnp.asarray(twist))
    tracers, velocity, sea = pl.pallas_call(
        finish_kernel,
        out_shape=(
            jax.ShapeDtypeStruct((16, ROWS, COLS), f32),
            jax.ShapeDtypeStruct((16, ROWS, COLS), f32),
            jax.ShapeDtypeStruct((ROWS, COLS), f32),
        ),
        in_specs=[hbm] * 5,
        out_specs=(hbm, hbm, hbm),
        scratch_shapes=[pltpu.SMEM((8,), f32), pltpu.VMEM((3, ROWS, COLS), f32), pltpu.VMEM((2, ROWS, COLS), f32), pltpu.VMEM((32, ROWS, COLS), f32), pltpu.VMEM((16, ROWS, COLS), f32), dma((4, 4)), dma((4, 2)), dma((4, 2)), dma((4,))],
        compiler_params=pltpu.CompilerParams(vmem_limit_bytes=67043328),
    )(thickness, planes, filt, flow, opens)
    shape = (2, 8, ROWS, COLS)
    return tracers.reshape(shape), velocity.reshape(shape), sea


def solution(mesh):
    return jax.shard_map(
        body,
        mesh=mesh,
        in_specs=(P(None, None, "lat", "lon"), P(), P(), P(None, "lat", "lon"), P("lat", "lon")),
        out_specs=(P(None, None, "lat", "lon"), P(None, None, "lat", "lon"), P("lat", "lon")),
        check_vma=False,
    )
```

```python
import functools
import math

import jax
import jax.numpy as jnp
import ml_dtypes
import numpy as np
from jax import lax
from jax.experimental import pallas as pl
from jax.experimental.pallas import tpu as pltpu
from jax.sharding import PartitionSpec as P

MESH = pl.DeviceIdType.MESH
SUB = 20
COEF = 0.65
NLAT = 1024
NLON = 3600
ROWS = 64
COLS = 450
PART = 8
EACH = ROWS // PART
TAKES = (13, 10, 0, 9)
STARTS = (0, 104, 184, 184)
LAG = 2
AHEAD = 6
HALO = 24
TILES = ((0, 128), (128, 256), (256, 384), (384, 450))
ROOT = math.sqrt(0.5)


def fourier_tables():
    k = np.arange(COLS)
    angle = 2.0 * np.pi * (np.outer(k, k) % COLS) / COLS
    both = np.zeros((512, 1024), np.float64)
    both[:COLS, :COLS] = np.cos(angle)
    both[:COLS, 512 : 512 + COLS] = np.sin(angle)
    high = both.astype(ml_dtypes.bfloat16)
    low = (both - high.astype(np.float64)).astype(ml_dtypes.bfloat16)
    twist = np.zeros((8, 512), np.float32)
    for j in range(1, 5):
        twist[2 * (j - 1), :COLS] = np.cos(2.0 * np.pi * j * k / NLON)
        twist[2 * (j - 1) + 1, :COLS] = np.sin(2.0 * np.pi * j * k / NLON)
    return np.stack([high, low]), twist


def place():
    lat = lax.axis_index("lat")
    lon = lax.axis_index("lon")
    ylo = lat // 8
    x = (lat % 8) // 2
    core = lat % 2
    xm = x + ylo * (3 - 2 * x)

    def peer(xm_to, lon_to):
        return {"lat": (ylo * 4 + xm_to + ylo * (3 - 2 * xm_to)) * 2 + core, "lon": lon_to}

    return lat, lon, ylo, core, xm, peer


def split_store(terms, j, cols, real, imag):
    value = jnp.concatenate([real, imag], axis=0)
    top = value.astype(jnp.bfloat16)
    terms[pl.ds(2 * PART * j, 2 * PART), cols] = top
    terms[pl.ds(10 * PART + 2 * PART * j, 2 * PART), cols] = (value - top.astype(jnp.float32)).astype(jnp.bfloat16)


def transform(c, base, recv, ybuf, cut_ref, cutb, tw_ref, wv, terms, acc):
    row_id = lax.broadcasted_iota(jnp.int32, (PART, 128), 0)
    cuts = jnp.zeros((PART, 128), jnp.int32)
    for r in range(PART):
        cuts = jnp.where(row_id == r, cut_ref[base + r], cuts)
    cutb[...] = cuts

    def product():
        both = jnp.dot(terms[...], wv[0], preferred_element_type=jnp.float32)
        fine = jnp.dot(terms[0 : 10 * PART, :], wv[1], preferred_element_type=jnp.float32)
        acc[...] = both[0 : 10 * PART] + both[10 * PART :] + fine

    def part(j, imag, cols):
        return acc[pl.ds(2 * PART * j + PART * imag, PART), cols]

    for lo, hi in TILES:
        cols = pl.ds(lo, hi - lo)
        x = [recv[c, d, :, cols] for d in range(8)]
        a = [x[d] + x[d + 4] for d in range(4)]
        b = [x[d] - x[d + 4] for d in range(4)]
        diff, total = ROOT * (b[1] - b[3]), ROOT * (b[1] + b[3])
        even, odd = a[0] + a[2], a[1] + a[3]
        real = {1: b[0] + diff, 2: a[0] - a[2], 3: b[0] - diff}
        imag = {1: -total - b[2], 2: a[3] - a[1], 3: b[2] - total}
        split_store(terms, 0, cols, even + odd, jnp.zeros_like(even))
        for j in range(1, 5):
            tc = tw_ref[2 * j - 2 : 2 * j - 1, lo:hi]
            ts = tw_ref[2 * j - 1 : 2 * j, lo:hi]
            if j < 4:
                split_store(terms, j, cols, real[j] * tc + imag[j] * ts, imag[j] * tc - real[j] * ts)
            else:
                split_store(terms, j, cols, (even - odd) * tc, (odd - even) * ts)
    product()
    for lo, hi in TILES:
        cols = pl.ds(lo, hi - lo)
        sines = pl.ds(512 + lo, hi - lo)
        limit = cutb[:, 0 : hi - lo]
        step = 8 * (lax.broadcasted_iota(jnp.int32, (PART, hi - lo), 1) + lo)
        for j in range(5):
            wave = step + j
            kept = jnp.minimum(wave, NLON - wave) <= limit
            scale = jnp.where(kept, (2.0 if 0 < j < 4 else 1.0) / NLON, 0.0)
            re = part(j, 0, cols) + part(j, 1, sines)
            im = part(j, 1, cols) - part(j, 0, sines)
            split_store(terms, j, cols, re * scale, im * scale)
    product()
    for lo, hi in TILES:
        cols = pl.ds(lo, hi - lo)
        sines = pl.ds(512 + lo, hi - lo)
        hr, hm = {}, {}
        for j in range(5):
            gr = part(j, 0, cols) - part(j, 1, sines)
            if j == 0:
                hr[0] = gr
                continue
            gi = part(j, 0, sines) + part(j, 1, cols)
            tc = tw_ref[2 * j - 2 : 2 * j - 1, lo:hi]
            ts = tw_ref[2 * j - 1 : 2 * j, lo:hi]
            hr[j] = gr * tc - gi * ts
            if j < 4:
                hm[j] = gr * ts + gi * tc
        even, odd = hr[0] + hr[4], hr[0] - hr[4]
        plain = [even + hr[2], odd - hm[2], even - hr[2], odd + hm[2]]
        turn = [
            hr[1] + hr[3],
            ROOT * (hr[1] - hm[1] - hr[3] - hm[3]),
            hm[3] - hm[1],
            ROOT * (hr[3] - hm[3] - hr[1] - hm[1]),
        ]
        for d in range(4):
            ybuf[c, d, :, cols] = plain[d] + turn[d]
            ybuf[c, d + 4, :, cols] = plain[d] - turn[d]


def assemble(store, offset, count, centre, left, right, tail):
    rows = pl.ds(offset, count)
    store[rows, 0:COLS] = centre
    tail[0:count, 0:66] = left
    lane = lax.broadcasted_iota(jnp.int32, (count, 128), 1)
    own = store[rows, 384:512]
    west = pltpu.roll(tail[0:count, :], 62, 1)
    east = pltpu.roll(right, 66, 1)
    store[rows, 384:512] = jnp.where(
        lane < 66, own, jnp.where(lane < 66 + HALO, east, jnp.where(lane >= 128 - HALO, west, 0.0))
    )


def exchange_kernel(
    f_ref, baro_in, land_in, cut_in, w_ref, tw_in,
    filt, flow, opens,
    baro, land, cut_ref, tw_ref, recv, ybuf, crecv, wv, terms, acc, cutb,
    state, masks, tail, held_flow, held_opens,
    lb, lm, rb_, rm, tb, tm, bb, bm, tlb, tlm, trb, trm, blb, blm, brb, brm,
    wsem, hsend, hrecv, rsem, osem, csend, crsem, dsend, fsem,
):
    lat, lon, ylo, core, xm, peer = place()
    lats, lons = 16, 8
    polar = xm == 0
    helper = (xm == 1) | (xm == 3)
    lat_up, lat_down = (lat + 1) % lats, (lat + lats - 1) % lats
    lon_up, lon_down = (lon + 1) % lons, (lon + lons - 1) % lons
    barrier = pltpu.get_barrier_semaphore()

    def greet(device):
        pl.semaphore_signal(barrier, 1, device_id=device, device_id_type=MESH)

    for lat_to in (lat, lat_up, lat_down):
        for lon_to in (lon, lon_up, lon_down):
            if lat_to is not lat or lon_to is not lon:
                greet({"lat": lat_to, "lon": lon_to})

    @pl.when(polar)
    def _():
        for k in range(lons):
            to = (lon + k) % lons
            if k:
                greet(peer(0, to))
            greet(peer(1, to))
            greet(peer(3, to))

    @pl.when(helper)
    def _():
        for k in range(lons):
            to = (lon + k) % lons
            if k:
                greet(peer(xm, to))
            greet(peer(0, to))

    near = [
        pltpu.make_async_copy(baro_in, baro, wsem.at[0]),
        pltpu.make_async_copy(land_in, land, wsem.at[1]),
    ]
    tables = [
        pltpu.make_async_copy(cut_in, cut_ref, wsem.at[2]),
        pltpu.make_async_copy(tw_in, tw_ref, wsem.at[3]),
        pltpu.make_async_copy(w_ref, wv, wsem.at[4]),
    ]
    for copy in near + tables:
        copy.start()
    terms[...] = jnp.zeros_like(terms)

    @pl.when(polar)
    def _():
        pl.semaphore_wait(barrier, 31)

    @pl.when(helper)
    def _():
        pl.semaphore_wait(barrier, 23)

    @pl.when(xm == 2)
    def _():
        pl.semaphore_wait(barrier, 8)

    def hop(i, source, target, **to):
        device = {"lat": lat, "lon": lon}
        device.update(to)
        return pltpu.make_async_remote_copy(source, target, hsend.at[i], hrecv.at[i], device_id=device, device_id_type=MESH)

    first = [
        hop(0, baro.at[:, :, pl.ds(384, 66)], lb, lon=lon_up),
        hop(1, land.at[:, pl.ds(384, 66)], lm, lon=lon_up),
        hop(2, baro.at[:, :, pl.ds(0, 128)], rb_, lon=lon_down),
        hop(3, land.at[:, pl.ds(0, 128)], rm, lon=lon_down),
        hop(4, baro.at[:, pl.ds(ROWS - HALO, HALO), :], tb, lat=lat_up),
        hop(5, land.at[pl.ds(ROWS - HALO, HALO), :], tm, lat=lat_up),
        hop(6, baro.at[:, pl.ds(0, HALO), :], bb, lat=lat_down),
        hop(7, land.at[pl.ds(0, HALO), :], bm, lat=lat_down),
    ]
    low_rows, top_rows = pl.ds(ROWS - HALO, HALO), pl.ds(0, HALO)
    west_cols, east_cols = pl.ds(384, 66), pl.ds(0, 128)
    corners = ((low_rows, lat_up, tlb, tlm, trb, trm), (top_rows, lat_down, blb, blm, brb, brm))
    for i, (part, lat_to, left, leftm, right, rightm) in enumerate(corners):
        first += [
            hop(8 + 4 * i, baro.at[:, part, west_cols], left, lat=lat_to, lon=lon_up),
            hop(9 + 4 * i, land.at[part, west_cols], leftm, lat=lat_to, lon=lon_up),
            hop(10 + 4 * i, baro.at[:, part, east_cols], right, lat=lat_to, lon=lon_down),
            hop(11 + 4 * i, land.at[part, east_cols], rightm, lat=lat_to, lon=lon_down),
        ]
    for copy in near:
        copy.wait()

    @pl.when(jnp.logical_not(polar))
    def _():
        for copy in first:
            copy.start()

    def chunk_of(xm_of, lon_of, i):
        unit = STARTS[xm_of] + lon_of * TAKES[xm_of] + i
        return unit // EACH, pl.ds(pl.multiple_of(unit % EACH * PART, PART), PART)

    def drain(chunks, sem):
        if chunks // EACH:
            whole = f_ref.at[pl.ds(0, chunks // EACH)]
            pltpu.make_async_copy(whole, whole, sem).wait()
        if chunks % EACH:
            rest = f_ref.at[0, pl.ds(0, chunks % EACH * PART), :]
            pltpu.make_async_copy(rest, rest, sem).wait()

    def send(i, xm_to, lon_to):
        plane, rows = chunk_of(xm_to, lon_to, i)
        pltpu.make_async_remote_copy(
            f_ref.at[plane, rows, :], recv.at[i, lon], osem, rsem.at[i], device_id=peer(xm_to, lon_to), device_id_type=MESH
        ).start()

    def deal_near(i):
        plane, rows = chunk_of(0, lon, i)
        pltpu.make_async_copy(f_ref.at[plane, rows, :], recv.at[i, lon], rsem.at[i]).start()

        def one(k, carry):
            send(i, 0, (lon + k) % lons)
            return carry

        lax.fori_loop(1, lons, one, 0)

    def deal_far(i, carry):
        def one(k, carry):
            to = (lon + k) % lons
            send(i, 1, to)

            @pl.when(i < TAKES[3])
            def _():
                send(i, 3, to)

            return carry

        return lax.fori_loop(0, lons, one, carry)

    @pl.when(polar)
    def _():
        deal_far(0, 0)
        for i in range(AHEAD):
            deal_near(i)
        lax.fori_loop(1, TAKES[1], deal_far, 0)
        for copy in first:
            copy.start()

    for copy in tables:
        copy.wait()

    base = ylo * 128 + core * ROWS
    far = xm // 2
    mine = jnp.where(polar, TAKES[0], jnp.where(helper, TAKES[1] + far * (TAKES[3] - TAKES[1]), 0))
    start = STARTS[1] + (STARTS[3] - STARTS[1]) * far

    def forward(i):
        pltpu.make_async_copy(crecv.at[0, pl.ds(0, 7)], crecv.at[0, pl.ds(0, 7)], crsem.at[i]).wait()

        def to_polar(source, origin):
            unit = start + origin * mine + i
            rows = pl.ds(pl.multiple_of(unit % EACH * PART, PART), PART)
            pltpu.make_async_remote_copy(
                source, filt.at[unit // EACH, rows, :], dsend, fsem, device_id=peer(0, lon), device_id_type=MESH
            ).start()

        to_polar(ybuf.at[i, lon], lon)

        def relay(k, carry):
            origin = (lon + k) % lons
            to_polar(crecv.at[i, origin], origin)
            return carry

        lax.fori_loop(1, lons, relay, 0)

    def chunk(i, carry):
        unit = jnp.where(polar, 0, start) + lon * mine + i
        plane = unit // EACH
        row = pl.multiple_of(unit % EACH * PART, PART)

        @pl.when(polar | helper)
        def _():
            pltpu.make_async_copy(recv.at[i], recv.at[i], rsem.at[i]).wait()
            transform(i, base + row, recv, ybuf, cut_ref, cutb, tw_ref, wv, terms, acc)

        @pl.when(polar)
        def _():
            target = filt.at[plane, pl.ds(row, PART), :]
            pltpu.make_async_copy(ybuf.at[i, lon], target, fsem).start()

            def back(k, carry):
                to = (lon + k) % lons
                pltpu.make_async_remote_copy(ybuf.at[i, to], target, csend, fsem, device_id=peer(0, to), device_id_type=MESH).start()
                return carry

            lax.fori_loop(1, lons, back, 0)

            @pl.when(i + AHEAD < TAKES[0])
            def _():
                deal_near(i + AHEAD)

        @pl.when(helper)
        def _():
            def swap(k, carry):
                to = (lon + k) % lons
                pltpu.make_async_remote_copy(
                    ybuf.at[i, to], crecv.at[i, lon], csend, crsem.at[i], device_id=peer(xm, to), device_id_type=MESH
                ).start()
                return carry

            lax.fori_loop(1, lons, swap, 0)

        @pl.when(helper & (i >= LAG))
        def _():
            forward(i - LAG)

        return carry

    lax.fori_loop(0, mine, chunk, 0)

    @pl.when(helper)
    def _():
        for i in range(LAG):
            forward(mine - LAG + i)

    for copy in first:
        copy.wait_recv()

    for i in range(3):
        assemble(state.at[i], 0, HALO, tb[i], tlb[i], trb[i], tail)
        assemble(state.at[i], HALO, ROWS, baro[i], lb[i], rb_[i], tail)
        assemble(state.at[i], HALO + ROWS, HALO, bb[i], blb[i], brb[i], tail)
    f32 = jnp.float32
    assemble(masks.at[0], 0, HALO, tm[...].astype(f32), tlm[...].astype(f32), trm[...].astype(f32), tail)
    assemble(masks.at[0], HALO, ROWS, land[...].astype(f32), lm[...].astype(f32), rm[...].astype(f32), tail)
    assemble(masks.at[0], HALO + ROWS, HALO, bm[...].astype(f32), blm[...].astype(f32), brm[...].astype(f32), tail)
    total = ROWS + 2 * HALO
    for r in range(0, total, 8):
        rows = pl.ds(r, 8)
        sea = masks[0, rows, :]
        below = masks[0, pl.ds(r + 1, 8), :] if r + 8 < total else sea
        east = sea * pltpu.roll(sea, 511, 1)
        row = (lax.broadcasted_iota(jnp.int32, (8, 512), 0) + (r + NLAT - HALO) + lat * ROWS) % NLAT
        north = jnp.where(row == NLAT - 1, 0.0, sea * below)
        masks[1, rows, :] = east
        masks[2, rows, :] = north
        state[1, rows, :] = state[1, rows, :] * east
        state[2, rows, :] = state[2, rows, :] * north

    def cycle(_, carry):
        for r in range(0, total, 8):
            rows = pl.ds(r, 8)
            e, n = state[1, rows, :], state[2, rows, :]
            above = state[2, pl.ds(r - 1, 8), :] if r else n
            div = e - pltpu.roll(e, 1, 1) + n - above
            state[0, rows, :] = state[0, rows, :] - (COEF * masks[0, rows, :]) * div
        for r in range(0, total, 8):
            rows = pl.ds(r, 8)
            s = state[0, rows, :]
            below = state[0, pl.ds(r + 1, 8), :] if r + 8 < total else s
            state[1, rows, :] = masks[1, rows, :] * (state[1, rows, :] - COEF * (pltpu.roll(s, 511, 1) - s))
            state[2, rows, :] = masks[2, rows, :] * (state[2, rows, :] - COEF * (below - s))
        return carry

    lax.fori_loop(0, SUB, cycle, 0)
    held_flow[...] = state[:, pl.ds(HALO, ROWS), 0:COLS]
    held_opens[...] = masks[1:3, pl.ds(HALO, ROWS), 0:COLS]
    made = [pltpu.make_async_copy(held_flow, flow, wsem.at[0]), pltpu.make_async_copy(held_opens, opens, wsem.at[1])]
    for copy in made:
        copy.start()

    for side in (1, 3):

        @pl.when(xm == side)
        def _():
            drain(7 * TAKES[side], csend)
            drain(8 * TAKES[side], dsend)

    @pl.when(polar)
    def _():
        drain(7 * TAKES[0] + 8 * TAKES[1] + 8 * TAKES[3], osem)
        drain(7 * TAKES[0], csend)
        drain(32 * EACH, fsem)

    for copy in made:
        copy.wait()
    for copy in first:
        copy.wait_send()


def finish_kernel(thick_in, f_ref, filt, flow_in, opens_in, tracers, velocity, sea, thick, flow, opens, block, made, isem, tsem, vsem, wsem):
    lat, lon, ylo, core, xm, peer = place()
    polar = xm == 0
    pieces = [(q, g) for q in range(4) for g in (2, 3, 0, 1)]

    def view(ref, q, g):
        return ref.at[pl.ds(8 * g, 8), pl.ds(16 * q, 16), :]

    def load(source):
        for q, g in pieces:
            pltpu.make_async_copy(view(source, q, g), view(block, q, g), isem.at[q, g]).start()

    @pl.when(polar)
    def _():
        load(filt)

    @pl.when(jnp.logical_not(polar))
    def _():
        load(f_ref)

    small = [pltpu.make_async_copy(flow_in, flow, wsem.at[0]), pltpu.make_async_copy(opens_in, opens, wsem.at[1]), pltpu.make_async_copy(thick_in, thick, wsem.at[3])]
    for copy in small:
        copy.start()
    for copy in small:
        copy.wait()
    weight = [thick[k] for k in range(8)]
    whole = functools.reduce(lambda a, b: a + b, weight)
    share = 1.0 / jnp.full((8, COLS), whole, jnp.float32)
    outs = [pltpu.make_async_copy(flow.at[0], sea, wsem.at[2])]
    outs[0].start()
    for q, g in pieces:
        pltpu.make_async_copy(view(f_ref, q, g), view(block, q, g), isem.at[q, g]).wait()
        if g < 2:
            outs.append(pltpu.make_async_copy(view(block, q, g), view(tracers, q, g), tsem.at[q, g]))
        else:
            c = g - 2
            for r in range(16 * q, 16 * q + 16, 8):
                rows = pl.ds(r, 8)
                level = [block[8 * g + k, rows, :] for k in range(8)]
                column = weight[0] * level[0]
                for k in range(1, 8):
                    column = column + weight[k] * level[k]
                column = flow[1 + c, rows, :] - column * share
                gate = opens[c, rows, :]
                for k in range(8):
                    made[8 * c + k, rows, :] = gate * (level[k] + column)
            outs.append(pltpu.make_async_copy(view(made, q, c), view(velocity, q, c), vsem.at[q, c]))
        outs[-1].start()
    for copy in outs:
        copy.wait()


def body(fields, thickness, cutoff, barotropic, land_sea):
    f32, i32, bf16 = jnp.float32, jnp.int32, jnp.bfloat16
    planes = fields.reshape(32, ROWS, COLS)
    table, twist = fourier_tables()
    hbm = pl.BlockSpec(memory_space=pltpu.HBM)
    dma = pltpu.SemaphoreType.DMA
    strips = []
    for rows in (ROWS,):
        strips += [pltpu.VMEM((3, rows, 66), f32), pltpu.VMEM((rows, 66), i32), pltpu.VMEM((3, rows, 128), f32), pltpu.VMEM((rows, 128), i32)]
    strips += [pltpu.VMEM((3, HALO, COLS), f32), pltpu.VMEM((HALO, COLS), i32)] * 2
    strips += [pltpu.VMEM((3, HALO, 66), f32), pltpu.VMEM((HALO, 66), i32), pltpu.VMEM((3, HALO, 128), f32), pltpu.VMEM((HALO, 128), i32)] * 2
    total = ROWS + 2 * HALO
    filt, flow, opens = pl.pallas_call(
        exchange_kernel,
        out_shape=(
            jax.ShapeDtypeStruct((32, ROWS, COLS), f32),
            jax.ShapeDtypeStruct((3, ROWS, COLS), f32),
            jax.ShapeDtypeStruct((2, ROWS, COLS), f32),
        ),
        in_specs=[hbm] * 6,
        out_specs=(hbm, hbm, hbm),
        scratch_shapes=[
            pltpu.VMEM((3, ROWS, COLS), f32),
            pltpu.VMEM((ROWS, COLS), i32),
            pltpu.SMEM((256,), i32),
            pltpu.VMEM((8, 512), f32),
            pltpu.VMEM((TAKES[0], 8, PART, COLS), f32),
            pltpu.VMEM((TAKES[0], 8, PART, COLS), f32),
            pltpu.VMEM((TAKES[1], 8, PART, COLS), f32),
            pltpu.VMEM((2, 512, 1024), bf16),
            pltpu.VMEM((20 * PART, 512), bf16),
            pltpu.VMEM((10 * PART, 1024), f32),
            pltpu.VMEM((PART, 128), i32),
            pltpu.VMEM((3, total, 512), f32),
            pltpu.VMEM((3, total, 512), f32),
            pltpu.VMEM((ROWS, 128), f32),
            pltpu.VMEM((3, ROWS, COLS), f32),
            pltpu.VMEM((2, ROWS, COLS), f32),
            *strips,
            dma((5,)), dma((16,)), dma((16,)), dma((TAKES[0],)), dma, dma, dma((TAKES[1],)), dma, dma,
        ],
        compiler_params=pltpu.CompilerParams(collective_id=1, has_side_effects=True, vmem_limit_bytes=67043328),
    )(planes, barotropic, land_sea, cutoff, jnp.asarray(table), jnp.asarray(twist))
    tracers, velocity, sea = pl.pallas_call(
        finish_kernel,
        out_shape=(
            jax.ShapeDtypeStruct((16, ROWS, COLS), f32),
            jax.ShapeDtypeStruct((16, ROWS, COLS), f32),
            jax.ShapeDtypeStruct((ROWS, COLS), f32),
        ),
        in_specs=[hbm] * 5,
        out_specs=(hbm, hbm, hbm),
        scratch_shapes=[pltpu.SMEM((8,), f32), pltpu.VMEM((3, ROWS, COLS), f32), pltpu.VMEM((2, ROWS, COLS), f32), pltpu.VMEM((32, ROWS, COLS), f32), pltpu.VMEM((16, ROWS, COLS), f32), dma((4, 4)), dma((4, 2)), dma((4, 2)), dma((4,))],
        compiler_params=pltpu.CompilerParams(vmem_limit_bytes=67043328),
    )(thickness, planes, filt, flow, opens)
    shape = (2, 8, ROWS, COLS)
    return tracers.reshape(shape), velocity.reshape(shape), sea


def solution(mesh):
    return jax.shard_map(
        body,
        mesh=mesh,
        in_specs=(P(None, None, "lat", "lon"), P(), P(), P(None, "lat", "lon"), P("lat", "lon")),
        out_specs=(P(None, None, "lat", "lon"), P(None, None, "lat", "lon"), P("lat", "lon")),
        check_vma=False,
    )
```

```python
import functools
import math

import jax
import jax.numpy as jnp
import ml_dtypes
import numpy as np
from jax import lax
from jax.experimental import pallas as pl
from jax.experimental.pallas import tpu as pltpu
from jax.sharding import PartitionSpec as P

MESH = pl.DeviceIdType.MESH
SUB = 20
COEF = 0.65
NLAT = 1024
NLON = 3600
ROWS = 64
COLS = 450
PART = 8
EACH = ROWS // PART
TAKES = (13, 10, 0, 9)
STARTS = (0, 104, 184, 184)
LAG = 3
AHEAD = 13
HALO = 24
TILES = ((0, 128), (128, 256), (256, 384), (384, 450))
ROOT = math.sqrt(0.5)


def fourier_tables():
    k = np.arange(COLS)
    angle = 2.0 * np.pi * (np.outer(k, k) % COLS) / COLS
    both = np.zeros((512, 1024), np.float64)
    both[:COLS, :COLS] = np.cos(angle)
    both[:COLS, 512 : 512 + COLS] = np.sin(angle)
    high = both.astype(ml_dtypes.bfloat16)
    low = (both - high.astype(np.float64)).astype(ml_dtypes.bfloat16)
    twist = np.zeros((8, 512), np.float32)
    for j in range(1, 5):
        twist[2 * (j - 1), :COLS] = np.cos(2.0 * np.pi * j * k / NLON)
        twist[2 * (j - 1) + 1, :COLS] = np.sin(2.0 * np.pi * j * k / NLON)
    return np.stack([high, low]), twist


def place():
    lat = lax.axis_index("lat")
    lon = lax.axis_index("lon")
    ylo = lat // 8
    x = (lat % 8) // 2
    core = lat % 2
    xm = x + ylo * (3 - 2 * x)

    def peer(xm_to, lon_to):
        return {"lat": (ylo * 4 + xm_to + ylo * (3 - 2 * xm_to)) * 2 + core, "lon": lon_to}

    return lat, lon, ylo, core, xm, peer


def split_store(terms, j, cols, real, imag):
    value = jnp.concatenate([real, imag], axis=0)
    top = value.astype(jnp.bfloat16)
    terms[pl.ds(2 * PART * j, 2 * PART), cols] = top
    terms[pl.ds(10 * PART + 2 * PART * j, 2 * PART), cols] = (value - top.astype(jnp.float32)).astype(jnp.bfloat16)


def transform(c, base, recv, ybuf, cut_ref, cutb, tw_ref, wv, terms, acc):
    row_id = lax.broadcasted_iota(jnp.int32, (PART, 128), 0)
    cuts = jnp.zeros((PART, 128), jnp.int32)
    for r in range(PART):
        cuts = jnp.where(row_id == r, cut_ref[base + r], cuts)
    cutb[...] = cuts

    def product():
        both = jnp.dot(terms[...], wv[0], preferred_element_type=jnp.float32)
        fine = jnp.dot(terms[0 : 10 * PART, :], wv[1], preferred_element_type=jnp.float32)
        acc[...] = both[0 : 10 * PART] + both[10 * PART :] + fine

    def part(j, imag, cols):
        return acc[pl.ds(2 * PART * j + PART * imag, PART), cols]

    for lo, hi in TILES:
        cols = pl.ds(lo, hi - lo)
        x = [recv[c, d, :, cols] for d in range(8)]
        a = [x[d] + x[d + 4] for d in range(4)]
        b = [x[d] - x[d + 4] for d in range(4)]
        diff, total = ROOT * (b[1] - b[3]), ROOT * (b[1] + b[3])
        even, odd = a[0] + a[2], a[1] + a[3]
        real = {1: b[0] + diff, 2: a[0] - a[2], 3: b[0] - diff}
        imag = {1: -total - b[2], 2: a[3] - a[1], 3: b[2] - total}
        split_store(terms, 0, cols, even + odd, jnp.zeros_like(even))
        for j in range(1, 5):
            tc = tw_ref[2 * j - 2 : 2 * j - 1, lo:hi]
            ts = tw_ref[2 * j - 1 : 2 * j, lo:hi]
            if j < 4:
                split_store(terms, j, cols, real[j] * tc + imag[j] * ts, imag[j] * tc - real[j] * ts)
            else:
                split_store(terms, j, cols, (even - odd) * tc, (odd - even) * ts)
    product()
    for lo, hi in TILES:
        cols = pl.ds(lo, hi - lo)
        sines = pl.ds(512 + lo, hi - lo)
        limit = cutb[:, 0 : hi - lo]
        step = 8 * (lax.broadcasted_iota(jnp.int32, (PART, hi - lo), 1) + lo)
        for j in range(5):
            wave = step + j
            kept = jnp.minimum(wave, NLON - wave) <= limit
            scale = jnp.where(kept, (2.0 if 0 < j < 4 else 1.0) / NLON, 0.0)
            re = part(j, 0, cols) + part(j, 1, sines)
            im = part(j, 1, cols) - part(j, 0, sines)
            split_store(terms, j, cols, re * scale, im * scale)
    product()
    for lo, hi in TILES:
        cols = pl.ds(lo, hi - lo)
        sines = pl.ds(512 + lo, hi - lo)
        hr, hm = {}, {}
        for j in range(5):
            gr = part(j, 0, cols) - part(j, 1, sines)
            if j == 0:
                hr[0] = gr
                continue
            gi = part(j, 0, sines) + part(j, 1, cols)
            tc = tw_ref[2 * j - 2 : 2 * j - 1, lo:hi]
            ts = tw_ref[2 * j - 1 : 2 * j, lo:hi]
            hr[j] = gr * tc - gi * ts
            if j < 4:
                hm[j] = gr * ts + gi * tc
        even, odd = hr[0] + hr[4], hr[0] - hr[4]
        plain = [even + hr[2], odd - hm[2], even - hr[2], odd + hm[2]]
        turn = [
            hr[1] + hr[3],
            ROOT * (hr[1] - hm[1] - hr[3] - hm[3]),
            hm[3] - hm[1],
            ROOT * (hr[3] - hm[3] - hr[1] - hm[1]),
        ]
        for d in range(4):
            ybuf[c, d, :, cols] = plain[d] + turn[d]
            ybuf[c, d + 4, :, cols] = plain[d] - turn[d]


def assemble(store, offset, count, centre, left, right, tail):
    rows = pl.ds(offset, count)
    store[rows, 0:COLS] = centre
    tail[0:count, 0:66] = left
    lane = lax.broadcasted_iota(jnp.int32, (count, 128), 1)
    own = store[rows, 384:512]
    west = pltpu.roll(tail[0:count, :], 62, 1)
    east = pltpu.roll(right, 66, 1)
    store[rows, 384:512] = jnp.where(
        lane < 66, own, jnp.where(lane < 66 + HALO, east, jnp.where(lane >= 128 - HALO, west, 0.0))
    )


def exchange_kernel(
    f_ref, baro_in, land_in, cut_in, w_ref, tw_in,
    filt, flow, opens,
    baro, land, cut_ref, tw_ref, recv, ybuf, crecv, wv, terms, acc, cutb,
    state, masks, tail, held_flow, held_opens,
    lb, lm, rb_, rm, tb, tm, bb, bm, tlb, tlm, trb, trm, blb, blm, brb, brm,
    wsem, hsend, hrecv, rsem, osem, csend, crsem, dsend, fsem,
):
    lat, lon, ylo, core, xm, peer = place()
    lats, lons = 16, 8
    polar = xm == 0
    helper = (xm == 1) | (xm == 3)
    lat_up, lat_down = (lat + 1) % lats, (lat + lats - 1) % lats
    lon_up, lon_down = (lon + 1) % lons, (lon + lons - 1) % lons
    barrier = pltpu.get_barrier_semaphore()

    def greet(device):
        pl.semaphore_signal(barrier, 1, device_id=device, device_id_type=MESH)

    for lat_to in (lat, lat_up, lat_down):
        for lon_to in (lon, lon_up, lon_down):
            if lat_to is not lat or lon_to is not lon:
                greet({"lat": lat_to, "lon": lon_to})

    @pl.when(polar)
    def _():
        for k in range(lons):
            to = (lon + k) % lons
            if k:
                greet(peer(0, to))
            greet(peer(1, to))
            greet(peer(3, to))

    @pl.when(helper)
    def _():
        for k in range(lons):
            to = (lon + k) % lons
            if k:
                greet(peer(xm, to))
            greet(peer(0, to))

    near = [
        pltpu.make_async_copy(baro_in, baro, wsem.at[0]),
        pltpu.make_async_copy(land_in, land, wsem.at[1]),
    ]
    tables = [
        pltpu.make_async_copy(cut_in, cut_ref, wsem.at[2]),
        pltpu.make_async_copy(tw_in, tw_ref, wsem.at[3]),
        pltpu.make_async_copy(w_ref, wv, wsem.at[4]),
    ]
    for copy in near + tables:
        copy.start()
    terms[...] = jnp.zeros_like(terms)

    @pl.when(polar)
    def _():
        pl.semaphore_wait(barrier, 31)

    @pl.when(helper)
    def _():
        pl.semaphore_wait(barrier, 23)

    @pl.when(xm == 2)
    def _():
        pl.semaphore_wait(barrier, 8)

    def hop(i, source, target, **to):
        device = {"lat": lat, "lon": lon}
        device.update(to)
        return pltpu.make_async_remote_copy(source, target, hsend.at[i], hrecv.at[i], device_id=device, device_id_type=MESH)

    first = [
        hop(0, baro.at[:, :, pl.ds(384, 66)], lb, lon=lon_up),
        hop(1, land.at[:, pl.ds(384, 66)], lm, lon=lon_up),
        hop(2, baro.at[:, :, pl.ds(0, 128)], rb_, lon=lon_down),
        hop(3, land.at[:, pl.ds(0, 128)], rm, lon=lon_down),
        hop(4, baro.at[:, pl.ds(ROWS - HALO, HALO), :], tb, lat=lat_up),
        hop(5, land.at[pl.ds(ROWS - HALO, HALO), :], tm, lat=lat_up),
        hop(6, baro.at[:, pl.ds(0, HALO), :], bb, lat=lat_down),
        hop(7, land.at[pl.ds(0, HALO), :], bm, lat=lat_down),
    ]
    low_rows, top_rows = pl.ds(ROWS - HALO, HALO), pl.ds(0, HALO)
    west_cols, east_cols = pl.ds(384, 66), pl.ds(0, 128)
    corners = ((low_rows, lat_up, tlb, tlm, trb, trm), (top_rows, lat_down, blb, blm, brb, brm))
    for i, (part, lat_to, left, leftm, right, rightm) in enumerate(corners):
        first += [
            hop(8 + 4 * i, baro.at[:, part, west_cols], left, lat=lat_to, lon=lon_up),
            hop(9 + 4 * i, land.at[part, west_cols], leftm, lat=lat_to, lon=lon_up),
            hop(10 + 4 * i, baro.at[:, part, east_cols], right, lat=lat_to, lon=lon_down),
            hop(11 + 4 * i, land.at[part, east_cols], rightm, lat=lat_to, lon=lon_down),
        ]
    for copy in near:
        copy.wait()

    @pl.when(jnp.logical_not(polar))
    def _():
        for copy in first:
            copy.start()

    def chunk_of(xm_of, lon_of, i):
        unit = STARTS[xm_of] + lon_of * TAKES[xm_of] + i
        return unit // EACH, pl.ds(pl.multiple_of(unit % EACH * PART, PART), PART)

    def drain(chunks, sem):
        if chunks // EACH:
            whole = f_ref.at[pl.ds(0, chunks // EACH)]
            pltpu.make_async_copy(whole, whole, sem).wait()
        if chunks % EACH:
            rest = f_ref.at[0, pl.ds(0, chunks % EACH * PART), :]
            pltpu.make_async_copy(rest, rest, sem).wait()

    def send(i, xm_to, lon_to):
        plane, rows = chunk_of(xm_to, lon_to, i)
        pltpu.make_async_remote_copy(
            f_ref.at[plane, rows, :], recv.at[i, lon], osem, rsem.at[i], device_id=peer(xm_to, lon_to), device_id_type=MESH
        ).start()

    def deal_near(i):
        plane, rows = chunk_of(0, lon, i)
        pltpu.make_async_copy(f_ref.at[plane, rows, :], recv.at[i, lon], rsem.at[i]).start()

        def one(k, carry):
            send(i, 0, (lon + k) % lons)
            return carry

        lax.fori_loop(1, lons, one, 0)

    def deal_far(i, carry):
        def one(k, carry):
            to = (lon + k) % lons
            send(i, 1, to)

            @pl.when(i < TAKES[3])
            def _():
                send(i, 3, to)

            return carry

        return lax.fori_loop(0, lons, one, carry)

    @pl.when(polar)
    def _():
        deal_far(0, 0)
        for i in range(AHEAD):
            deal_near(i)
        lax.fori_loop(1, TAKES[1], deal_far, 0)
        for copy in first:
            copy.start()

    for copy in tables:
        copy.wait()

    base = ylo * 128 + core * ROWS
    far = xm // 2
    mine = jnp.where(polar, TAKES[0], jnp.where(helper, TAKES[1] + far * (TAKES[3] - TAKES[1]), 0))
    start = STARTS[1] + (STARTS[3] - STARTS[1]) * far

    def forward(i):
        pltpu.make_async_copy(crecv.at[0, pl.ds(0, 7)], crecv.at[0, pl.ds(0, 7)], crsem.at[i]).wait()

        def to_polar(source, origin):
            unit = start + origin * mine + i
            rows = pl.ds(pl.multiple_of(unit % EACH * PART, PART), PART)
            pltpu.make_async_remote_copy(
                source, filt.at[unit // EACH, rows, :], dsend, fsem, device_id=peer(0, lon), device_id_type=MESH
            ).start()

        to_polar(ybuf.at[i, lon], lon)

        def relay(k, carry):
            origin = (lon + k) % lons
            to_polar(crecv.at[i, origin], origin)
            return carry

        lax.fori_loop(1, lons, relay, 0)

    def chunk(i, carry):
        unit = jnp.where(polar, 0, start) + lon * mine + i
        plane = unit // EACH
        row = pl.multiple_of(unit % EACH * PART, PART)

        @pl.when(polar | helper)
        def _():
            pltpu.make_async_copy(recv.at[i], recv.at[i], rsem.at[i]).wait()
            transform(i, base + row, recv, ybuf, cut_ref, cutb, tw_ref, wv, terms, acc)

        @pl.when(polar)
        def _():
            target = filt.at[plane, pl.ds(row, PART), :]
            pltpu.make_async_copy(ybuf.at[i, lon], target, fsem).start()

            def back(k, carry):
                to = (lon + k) % lons
                pltpu.make_async_remote_copy(ybuf.at[i, to], target, csend, fsem, device_id=peer(0, to), device_id_type=MESH).start()
                return carry

            lax.fori_loop(1, lons, back, 0)

            @pl.when(i + AHEAD < TAKES[0])
            def _():
                deal_near(i + AHEAD)

        @pl.when(helper)
        def _():
            def swap(k, carry):
                to = (lon + k) % lons
                pltpu.make_async_remote_copy(
                    ybuf.at[i, to], crecv.at[i, lon], csend, crsem.at[i], device_id=peer(xm, to), device_id_type=MESH
                ).start()
                return carry

            lax.fori_loop(1, lons, swap, 0)

        @pl.when(helper & (i >= LAG))
        def _():
            forward(i - LAG)

        return carry

    lax.fori_loop(0, mine, chunk, 0)

    @pl.when(helper)
    def _():
        for i in range(LAG):
            forward(mine - LAG + i)

    for copy in first:
        copy.wait_recv()

    for i in range(3):
        assemble(state.at[i], 0, HALO, tb[i], tlb[i], trb[i], tail)
        assemble(state.at[i], HALO, ROWS, baro[i], lb[i], rb_[i], tail)
        assemble(state.at[i], HALO + ROWS, HALO, bb[i], blb[i], brb[i], tail)
    f32 = jnp.float32
    assemble(masks.at[0], 0, HALO, tm[...].astype(f32), tlm[...].astype(f32), trm[...].astype(f32), tail)
    assemble(masks.at[0], HALO, ROWS, land[...].astype(f32), lm[...].astype(f32), rm[...].astype(f32), tail)
    assemble(masks.at[0], HALO + ROWS, HALO, bm[...].astype(f32), blm[...].astype(f32), brm[...].astype(f32), tail)
    total = ROWS + 2 * HALO
    for r in range(0, total, 8):
        rows = pl.ds(r, 8)
        sea = masks[0, rows, :]
        below = masks[0, pl.ds(r + 1, 8), :] if r + 8 < total else sea
        east = sea * pltpu.roll(sea, 511, 1)
        row = (lax.broadcasted_iota(jnp.int32, (8, 512), 0) + (r + NLAT - HALO) + lat * ROWS) % NLAT
        north = jnp.where(row == NLAT - 1, 0.0, sea * below)
        masks[1, rows, :] = east
        masks[2, rows, :] = north
        state[1, rows, :] = state[1, rows, :] * east
        state[2, rows, :] = state[2, rows, :] * north

    def cycle(_, carry):
        for r in range(0, total, 8):
            rows = pl.ds(r, 8)
            e, n = state[1, rows, :], state[2, rows, :]
            above = state[2, pl.ds(r - 1, 8), :] if r else n
            div = e - pltpu.roll(e, 1, 1) + n - above
            state[0, rows, :] = state[0, rows, :] - (COEF * masks[0, rows, :]) * div
        for r in range(0, total, 8):
            rows = pl.ds(r, 8)
            s = state[0, rows, :]
            below = state[0, pl.ds(r + 1, 8), :] if r + 8 < total else s
            state[1, rows, :] = masks[1, rows, :] * (state[1, rows, :] - COEF * (pltpu.roll(s, 511, 1) - s))
            state[2, rows, :] = masks[2, rows, :] * (state[2, rows, :] - COEF * (below - s))
        return carry

    lax.fori_loop(0, SUB, cycle, 0)
    held_flow[...] = state[:, pl.ds(HALO, ROWS), 0:COLS]
    held_opens[...] = masks[1:3, pl.ds(HALO, ROWS), 0:COLS]
    made = [pltpu.make_async_copy(held_flow, flow, wsem.at[0]), pltpu.make_async_copy(held_opens, opens, wsem.at[1])]
    for copy in made:
        copy.start()

    for side in (1, 3):

        @pl.when(xm == side)
        def _():
            drain(7 * TAKES[side], csend)
            drain(8 * TAKES[side], dsend)

    @pl.when(polar)
    def _():
        drain(7 * TAKES[0] + 8 * TAKES[1] + 8 * TAKES[3], osem)
        drain(7 * TAKES[0], csend)
        drain(32 * EACH, fsem)

    for copy in made:
        copy.wait()
    for copy in first:
        copy.wait_send()


def finish_kernel(thick_in, f_ref, filt, flow_in, opens_in, tracers, velocity, sea, thick, flow, opens, block, made, isem, tsem, vsem, wsem):
    lat, lon, ylo, core, xm, peer = place()
    polar = xm == 0
    pieces = [(q, g) for q in range(4) for g in (2, 3, 0, 1)]

    def view(ref, q, g):
        return ref.at[pl.ds(8 * g, 8), pl.ds(16 * q, 16), :]

    def load(source):
        for q, g in pieces:
            pltpu.make_async_copy(view(source, q, g), view(block, q, g), isem.at[q, g]).start()

    @pl.when(polar)
    def _():
        load(filt)

    @pl.when(jnp.logical_not(polar))
    def _():
        load(f_ref)

    small = [pltpu.make_async_copy(flow_in, flow, wsem.at[0]), pltpu.make_async_copy(opens_in, opens, wsem.at[1]), pltpu.make_async_copy(thick_in, thick, wsem.at[3])]
    for copy in small:
        copy.start()
    for copy in small:
        copy.wait()
    weight = [thick[k] for k in range(8)]
    whole = functools.reduce(lambda a, b: a + b, weight)
    share = 1.0 / jnp.full((8, COLS), whole, jnp.float32)
    outs = [pltpu.make_async_copy(flow.at[0], sea, wsem.at[2])]
    outs[0].start()
    for q, g in pieces:
        pltpu.make_async_copy(view(f_ref, q, g), view(block, q, g), isem.at[q, g]).wait()
        if g < 2:
            outs.append(pltpu.make_async_copy(view(block, q, g), view(tracers, q, g), tsem.at[q, g]))
        else:
            c = g - 2
            for r in range(16 * q, 16 * q + 16, 8):
                rows = pl.ds(r, 8)
                level = [block[8 * g + k, rows, :] for k in range(8)]
                column = weight[0] * level[0]
                for k in range(1, 8):
                    column = column + weight[k] * level[k]
                column = flow[1 + c, rows, :] - column * share
                gate = opens[c, rows, :]
                for k in range(8):
                    made[8 * c + k, rows, :] = gate * (level[k] + column)
            outs.append(pltpu.make_async_copy(view(made, q, c), view(velocity, q, c), vsem.at[q, c]))
        outs[-1].start()
    for copy in outs:
        copy.wait()


def body(fields, thickness, cutoff, barotropic, land_sea):
    f32, i32, bf16 = jnp.float32, jnp.int32, jnp.bfloat16
    planes = fields.reshape(32, ROWS, COLS)
    table, twist = fourier_tables()
    hbm = pl.BlockSpec(memory_space=pltpu.HBM)
    dma = pltpu.SemaphoreType.DMA
    strips = []
    for rows in (ROWS,):
        strips += [pltpu.VMEM((3, rows, 66), f32), pltpu.VMEM((rows, 66), i32), pltpu.VMEM((3, rows, 128), f32), pltpu.VMEM((rows, 128), i32)]
    strips += [pltpu.VMEM((3, HALO, COLS), f32), pltpu.VMEM((HALO, COLS), i32)] * 2
    strips += [pltpu.VMEM((3, HALO, 66), f32), pltpu.VMEM((HALO, 66), i32), pltpu.VMEM((3, HALO, 128), f32), pltpu.VMEM((HALO, 128), i32)] * 2
    total = ROWS + 2 * HALO
    filt, flow, opens = pl.pallas_call(
        exchange_kernel,
        out_shape=(
            jax.ShapeDtypeStruct((32, ROWS, COLS), f32),
            jax.ShapeDtypeStruct((3, ROWS, COLS), f32),
            jax.ShapeDtypeStruct((2, ROWS, COLS), f32),
        ),
        in_specs=[hbm] * 6,
        out_specs=(hbm, hbm, hbm),
        scratch_shapes=[
            pltpu.VMEM((3, ROWS, COLS), f32),
            pltpu.VMEM((ROWS, COLS), i32),
            pltpu.SMEM((256,), i32),
            pltpu.VMEM((8, 512), f32),
            pltpu.VMEM((TAKES[0], 8, PART, COLS), f32),
            pltpu.VMEM((TAKES[0], 8, PART, COLS), f32),
            pltpu.VMEM((TAKES[1], 8, PART, COLS), f32),
            pltpu.VMEM((2, 512, 1024), bf16),
            pltpu.VMEM((20 * PART, 512), bf16),
            pltpu.VMEM((10 * PART, 1024), f32),
            pltpu.VMEM((PART, 128), i32),
            pltpu.VMEM((3, total, 512), f32),
            pltpu.VMEM((3, total, 512), f32),
            pltpu.VMEM((ROWS, 128), f32),
            pltpu.VMEM((3, ROWS, COLS), f32),
            pltpu.VMEM((2, ROWS, COLS), f32),
            *strips,
            dma((5,)), dma((16,)), dma((16,)), dma((TAKES[0],)), dma, dma, dma((TAKES[1],)), dma, dma,
        ],
        compiler_params=pltpu.CompilerParams(collective_id=1, has_side_effects=True, vmem_limit_bytes=67043328),
    )(planes, barotropic, land_sea, cutoff, jnp.asarray(table), jnp.asarray(twist))
    tracers, velocity, sea = pl.pallas_call(
        finish_kernel,
        out_shape=(
            jax.ShapeDtypeStruct((16, ROWS, COLS), f32),
            jax.ShapeDtypeStruct((16, ROWS, COLS), f32),
            jax.ShapeDtypeStruct((ROWS, COLS), f32),
        ),
        in_specs=[hbm] * 5,
        out_specs=(hbm, hbm, hbm),
        scratch_shapes=[pltpu.SMEM((8,), f32), pltpu.VMEM((3, ROWS, COLS), f32), pltpu.VMEM((2, ROWS, COLS), f32), pltpu.VMEM((32, ROWS, COLS), f32), pltpu.VMEM((16, ROWS, COLS), f32), dma((4, 4)), dma((4, 2)), dma((4, 2)), dma((4,))],
        compiler_params=pltpu.CompilerParams(vmem_limit_bytes=67043328),
    )(thickness, planes, filt, flow, opens)
    shape = (2, 8, ROWS, COLS)
    return tracers.reshape(shape), velocity.reshape(shape), sea


def solution(mesh):
    return jax.shard_map(
        body,
        mesh=mesh,
        in_specs=(P(None, None, "lat", "lon"), P(), P(), P(None, "lat", "lon"), P("lat", "lon")),
        out_specs=(P(None, None, "lat", "lon"), P(None, None, "lat", "lon"), P("lat", "lon")),
        check_vma=False,
    )
```
